128 devices in a mesh: row: 2 (over x_lo), col: 64 (over z, y, x_hi, core).
Axes of the slice: x: 4 (x_hi: 2, x_lo: 2; x = x_hi * 2 + x_lo), y: 4, z: 4, core: 2. Of those that a mesh axis runs over, the one named last changes fastest.
Arguments:
- panel: bfloat16 [196608, 1024], P('col', 'row'), may hold values from -0.1875 to 0.1875
- rhs: float32 [1024, 196608], P('row', 'col'), may hold values from -6 to 6
- diag_inverse: bfloat16 [2, 512, 512], replicated, may hold values from -1 to 2, as said below
Outputs:
- solved: bfloat16 [1024, 1024], P(None, 'row')
- updated: float32 [1024, 196608], P('row', 'col')
The draws below stay inside these ranges and needn't reach their ends.
Inputs may be any that keep to these rules, and one draw needn't show every extreme that they name: `diag_inverse`: each block is lower triangular; its diagonal entries are 0.5 or more.
All inputs are finite; a program needn't handle non-finite values.
Results may differ from the reference program's by a relative error of at most 0.0065.
Values may be sent and summed in bfloat16 or wider, within the bound.
A program may use at most 128 MiB of HBM per device.

```python
import jax
import jax.numpy as jnp
from jax import lax

NB = 512
NBR_DEV = 6
NRHS = 1024
STEPS = 2
N = 196608


def draw_diag_inverse(key, part):
    base = jax.random.fold_in(key, 11)
    first_key, second_key = jax.random.split(base)
    spread = jnp.clip(jax.random.normal(first_key, (STEPS, NB, NB), jnp.float32), -3.0, 3.0)
    diagonal = jax.random.uniform(second_key, (STEPS, NB), jnp.float32, 0.6, 1.6)
    lower = jnp.tril(spread, -1) / jnp.sqrt(jnp.float32(NB))
    whole = lower + jnp.eye(NB, dtype=jnp.float32)[None, :, :] * diagonal[:, :, None]
    return whole.astype(jnp.bfloat16)


def block_levels(stream_key, shape, cuts, smallest, top_value):
    def one(dim, blocks):
        steps = jax.random.uniform(jax.random.fold_in(jax.random.fold_in(stream_key, 6), dim), (blocks,), jnp.float32, smallest / len(cuts), top_value / len(cuts))
        return jnp.repeat(jnp.exp(steps), shape[dim] // blocks).reshape((-1,) + (1,) * (len(shape) - dim - 1))

    gain = one(*cuts[0])
    for cut in cuts[1:]:
        gain = gain * one(*cut)
    return gain


def bell_draw(stream_key, extent, scale, most, cuts=(), held_as=jnp.bfloat16):
    drawn = scale * jax.random.normal(stream_key, extent, jnp.float32)
    if cuts:
        drawn = drawn * block_levels(stream_key, extent, cuts, -0.22, 0.18)
    return jnp.clip(drawn, -most, most).astype(held_as)


def setup_inputs(seed: int = 0) -> dict:
    keys = jax.random.split(jax.random.key(seed), 4)
    panel = bell_draw(keys[0], (N, STEPS * NB), (STEPS * NB) ** -0.5, 0.1875, ((0, 64), (1, 2)))
    rhs = bell_draw(keys[1], (NRHS, N), 1.0, 6.0, ((0, 2), (1, 64)), jnp.float32)
    diag_inverse = draw_diag_inverse(jax.random.fold_in(keys[3], 71), 0)
    return dict(panel=panel, rhs=rhs, diag_inverse=diag_inverse)


def reference(panel, rhs, diag_inverse):
    rows_dev = NBR_DEV * NB
    masked = panel
    for current in range(STEPS):
        start = current * rows_dev
        masked = masked.at[start:start + NB, current * NB:].set(jnp.zeros((), jnp.bfloat16))
    pieces = []
    for current in range(STEPS):
        start = current * rows_dev
        residual = rhs[:, start:start + NB]
        if current > 0:
            earlier = jnp.concatenate(pieces, axis=1)
            factor_rows = masked[start:start + NB, 0:current * NB]
            products = lax.dot_general(earlier, factor_rows, (((1,), (1,)), ((), ())), preferred_element_type=jnp.float32)
            residual = residual - products
        inverse = diag_inverse[current].astype(jnp.float32)
        solution = jnp.dot(residual, inverse.T, precision=lax.Precision.HIGHEST)
        pieces.append(solution.astype(jnp.bfloat16))
    solved = jnp.concatenate(pieces, axis=1)
    window = lax.dot_general(solved, masked, (((1,), (1,)), ((), ())), preferred_element_type=jnp.float32)
    updated = rhs - window
    return solved, updated
```

```python
import functools

import jax
import jax.numpy as jnp
from jax import lax
from jax.experimental import pallas as pl
from jax.experimental.pallas import tpu as pltpu
from jax.sharding import PartitionSpec as P

MESH = pl.DeviceIdType.MESH
NT = (((1,), (1,)), ((), ()))
SIDE = 4
PIECES = SIDE * SIDE
CHUNK = 256
FIRST = 4


def remote(src, dst, send, recv, row, col):
    return pltpu.make_async_remote_copy(
        src_ref=src, dst_ref=dst, send_sem=send, recv_sem=recv,
        device_id=(row, col), device_id_type=MESH,
    )


def kernel(
    panel, rhs, inverse, updated, solved,
    own, other, work, mine, cross, made, before, inv,
    panel_send, panel_recv, scatter_send, scatter_recv, before_send, before_recv,
    x_send, x_recv, y_send, y_recv, z_send, z_recv, core_send, core_recv,
    load_sem, store_sem, solved_sem,
):
    block = inv.shape[0]
    rows_dev = own.shape[0]
    chunks = rows_dev // CHUNK
    row = lax.axis_index("row")
    col = lax.axis_index("col")
    core = lax.rem(col, 2)
    x_hi = lax.rem(col // 2, 2)
    piece = col // 4
    y = lax.rem(piece, SIDE)
    z = piece // SIDE
    length = block // PIECES
    plane = length * SIDE
    has_cross = core == row

    def at(z_, y_, x_, core_):
        return ((z_ * SIDE + y_) * 2 + x_) * 2 + core_

    load_own = pltpu.make_async_copy(panel, own, load_sem.at[0])
    load_first = pltpu.make_async_copy(
        rhs.at[:, pl.ds(0, block)], work.at[:, pl.ds(0, block)], load_sem.at[1]
    )
    load_rest = pltpu.make_async_copy(
        rhs.at[:, pl.ds(block, rows_dev - block)],
        work.at[:, pl.ds(block, rows_dev - block)],
        load_sem.at[2],
    )
    load_inv = pltpu.make_async_copy(inverse.at[core], inv, load_sem.at[3])
    load_first.start()

    @pl.when(col < 2)
    def _():
        load_inv.start()

    barrier = pltpu.get_barrier_semaphore()

    def greet(row_, col_):
        pl.semaphore_signal(barrier, inc=1, device_id=(row_, col_), device_id_type=MESH)

    greet(1 - row, col)
    greet(row, at(z, y, x_hi, 1 - core))
    greet(row, at(z, y, 1 - x_hi, core))
    greet(1 - row, at(z, y, 1 - x_hi, core))
    for d in range(1, SIDE):
        greet(row, at(z, lax.rem(y + d, SIDE), x_hi, core))
        greet(row, at(lax.rem(z + d, SIDE), y, x_hi, core))

    @pl.when(col < 2)
    def _():
        @pl.loop(1, PIECES)
        def _(p):
            greet(row, p * 4 + core)

    @pl.when((x_hi == 0) & (piece > 0))
    def _():
        greet(row, core)

    pl.semaphore_wait(
        barrier,
        10 + jnp.where(col < 2, PIECES - 1, 0) + jnp.where((x_hi == 0) & (piece > 0), 1, 0),
    )

    def panel_copy(j):
        part = pl.ds(pl.multiple_of(j * CHUNK, CHUNK), CHUNK)
        return remote(
            panel.at[part], other.at[part], panel_send.at[j], panel_recv.at[j], 1 - row, col
        )

    @pl.loop(0, FIRST)
    def _(j):
        panel_copy(j).start()

    load_own.start()
    load_rest.start()
    load_first.wait()
    load_own.wait()
    load_rest.wait()

    before_copy = remote(made, before, before_send, before_recv, row, 1)

    def scatter_copy(p):
        part = pl.ds(pl.multiple_of(p * length, length), length)
        return remote(
            made.at[part], mine.at[core, part], scatter_send.at[p], scatter_recv, row, p * 4 + core
        )

    def solve(factor):
        @pl.loop(0, 4)
        def _(i):
            tall = block // 4
            part = pl.ds(pl.multiple_of(i * tall, tall), tall)
            rest = work[part, :block]
            if factor is not None:
                rest = rest - lax.dot_general(
                    before[part, :], factor[:block, :], NT, preferred_element_type=jnp.float32
                )
            top = rest.astype(jnp.bfloat16)
            rest = rest - top.astype(jnp.float32)
            middle = rest.astype(jnp.bfloat16)
            low = (rest - middle.astype(jnp.float32)).astype(jnp.bfloat16)
            total = lax.dot_general(low, inv[...], NT, preferred_element_type=jnp.float32)
            total += lax.dot_general(middle, inv[...], NT, preferred_element_type=jnp.float32)
            total += lax.dot_general(top, inv[...], NT, preferred_element_type=jnp.float32)
            made[part, :] = total.astype(jnp.bfloat16)

    @pl.when(col < 2)
    def _():
        load_inv.wait()

        @pl.when(col == 0)
        def _():
            solve(None)
            before_copy.start()

        @pl.when(col == 1)
        def _():
            before_copy.wait_recv()

            @pl.when(row == 0)
            def _():
                solve(own)

            @pl.when(row == 1)
            def _():
                for j in range(block // CHUNK):
                    panel_copy(j).wait_recv()
                solve(other)

        @pl.loop(1, PIECES)
        def _(p):
            scatter_copy(p).start()

        mine[core, :length, :] = made[:length, :]

    def spot(p, count=1):
        return pl.ds(pl.multiple_of(p * length, length), length * count)

    here = spot(piece)
    x_across = remote(
        mine.at[core, here], mine.at[core, here], x_send.at[0], x_recv.at[0], row, at(z, y, 1, core)
    )
    x_cross = [
        remote(
            mine.at[core, here], cross.at[here], x_send.at[1 + i], x_recv.at[1],
            1 - row, at(z, y, i, core),
        )
        for i in range(2)
    ]

    @pl.when(x_hi == 0)
    def _():
        @pl.when(piece > 0)
        def _():
            scatter_copy(piece).wait_recv()

        x_across.start()

        @pl.when(~has_cross)
        def _():
            for copy in x_cross:
                copy.start()

    @pl.loop(FIRST, chunks)
    def _(j):
        panel_copy(j).start()

    @pl.when(x_hi == 1)
    def _():
        x_across.wait_recv()

    def y_copy(which, buffer, d, p):
        return remote(
            buffer.at[spot(p)], buffer.at[spot(p)], y_send.at[which, d - 1], y_recv.at[which, d - 1],
            row, at(z, lax.rem(y + d, SIDE), x_hi, core),
        )

    def z_copy(which, buffer, d, p):
        return remote(
            buffer.at[spot(p, SIDE)], buffer.at[spot(p, SIDE)],
            z_send.at[which, d - 1], z_recv.at[which, d - 1],
            row, at(lax.rem(z + d, SIDE), y, x_hi, core),
        )

    own_half = mine.at[core]
    for d in range(1, SIDE):
        y_copy(0, own_half, d, piece).start()

    @pl.when(has_cross)
    def _():
        x_cross[0].wait_recv()
        for d in range(1, SIDE):
            y_copy(1, cross, d, piece).start()

    def y_from(d):
        return z * SIDE + lax.rem(y + SIDE - d, SIDE)

    def z_from(d):
        return lax.rem(z + SIDE - d, SIDE) * SIDE

    for d in range(1, SIDE):
        y_copy(0, own_half, d, y_from(d)).wait_recv()
    for d in range(1, SIDE):
        z_copy(0, own_half, d, z * SIDE).start()

    @pl.when(has_cross)
    def _():
        for d in range(1, SIDE):
            y_copy(1, cross, d, y_from(d)).wait_recv()
        for d in range(1, SIDE):
            z_copy(1, cross, d, z * SIDE).start()

    buddy = at(z, y, x_hi, 1 - core)
    give = remote(own_half, own_half, core_send.at[0], core_recv.at[0], row, buddy)
    theirs = mine.at[1 - core]
    take = remote(theirs, theirs, core_send.at[0], core_recv.at[0], row, buddy)
    share_cross = remote(cross, cross, core_send.at[1], core_recv.at[1], row, buddy)

    for d in range(1, SIDE):
        z_copy(0, own_half, d, z_from(d)).wait_recv()
    give.start()

    @pl.when(has_cross)
    def _():
        for d in range(1, SIDE):
            z_copy(1, cross, d, z_from(d)).wait_recv()
        share_cross.start()

    take.wait_recv()

    @pl.when(~has_cross)
    def _():
        share_cross.wait_recv()

    put_mine = pltpu.make_async_copy(
        mine.at[row], solved.at[pl.ds(pl.multiple_of(row * block, block), block)], solved_sem.at[0]
    )
    put_cross = pltpu.make_async_copy(
        cross, solved.at[pl.ds(pl.multiple_of((1 - row) * block, block), block)], solved_sem.at[1]
    )
    put_mine.start()
    put_cross.start()

    @pl.when((col < 2) & (row >= col))
    def _():
        own[:block, :] = jnp.zeros((block, own.shape[1]), own.dtype)

    @pl.when(~((col == 1) & (row == 1)))
    def _():
        for j in range(block // CHUNK):
            panel_copy(j).wait_recv()

    @pl.when((col < 2) & (1 - row >= col))
    def _():
        other[:block, :] = jnp.zeros((block, other.shape[1]), other.dtype)

    def store(j):
        part = pl.ds(pl.multiple_of(j * CHUNK, CHUNK), CHUNK)
        return pltpu.make_async_copy(work.at[:, part], updated.at[:, part], store_sem.at[j])

    def update(j):
        part = pl.ds(pl.multiple_of(j * CHUNK, CHUNK), CHUNK)
        total = lax.dot_general(
            mine[row], own[part, :], NT, preferred_element_type=jnp.float32
        )
        total += lax.dot_general(
            mine[1 - row], other[part, :], NT, preferred_element_type=jnp.float32
        )
        work[:, part] -= total
        store(j).start()

    @pl.loop(0, block // CHUNK)
    def _(j):
        update(j)

    @pl.loop(block // CHUNK, chunks)
    def _(j):
        panel_copy(j).wait_recv()
        update(j)

    @pl.loop(0, chunks)
    def _(j):
        panel_copy(j).wait_send()
        store(j).wait()

    put_mine.wait()
    put_cross.wait()
    give.wait_send()
    for d in range(1, SIDE):
        y_copy(0, own_half, d, piece).wait_send()
        z_copy(0, own_half, d, z * SIDE).wait_send()

    @pl.when(has_cross)
    def _():
        share_cross.wait_send()
        for d in range(1, SIDE):
            y_copy(1, cross, d, piece).wait_send()
            z_copy(1, cross, d, z * SIDE).wait_send()

    @pl.when(x_hi == 0)
    def _():
        x_across.wait_send()

        @pl.when(~has_cross)
        def _():
            for copy in x_cross:
                copy.wait_send()

    @pl.when(col < 2)
    def _():
        @pl.when(col == 0)
        def _():
            before_copy.wait_send()

        @pl.loop(1, PIECES)
        def _(p):
            scatter_copy(p).wait_send()


def shards(panel, rhs, inverse):
    rows_dev, width = panel.shape
    half = rhs.shape[0]
    block = inverse.shape[1]
    chunks = rows_dev // CHUNK
    any_space = pl.BlockSpec(memory_space=pl.ANY)
    dma = pltpu.SemaphoreType.DMA
    updated, solved = pl.pallas_call(
        kernel,
        out_shape=(
            jax.ShapeDtypeStruct(rhs.shape, jnp.float32),
            jax.ShapeDtypeStruct((2 * half, block), jnp.bfloat16),
        ),
        in_specs=[any_space] * 3,
        out_specs=(any_space, any_space),
        scratch_shapes=[
            pltpu.VMEM((rows_dev, width), jnp.bfloat16),
            pltpu.VMEM((rows_dev, width), jnp.bfloat16),
            pltpu.VMEM(rhs.shape, jnp.float32),
            pltpu.VMEM((2, half, block), jnp.bfloat16),
            pltpu.VMEM((half, block), jnp.bfloat16),
            pltpu.VMEM((half, block), jnp.bfloat16),
            pltpu.VMEM((half, block), jnp.bfloat16),
            pltpu.VMEM((block, block), jnp.bfloat16),
            dma((chunks,)), dma((chunks,)), dma((PIECES,)), dma, dma, dma,
            dma((3,)), dma((2,)), dma((2, 3)), dma((2, 3)), dma((2, 3)), dma((2, 3)),
            dma((2,)), dma((2,)),
            dma((4,)), dma((chunks,)), dma((2,)),
        ],
        compiler_params=pltpu.CompilerParams(collective_id=0, has_side_effects=True),
        name="window",
    )(panel, rhs, inverse)
    return solved, updated


def solution(mesh):
    return jax.shard_map(
        shards,
        mesh=mesh,
        in_specs=(P("col", "row"), P("row", "col"), P()),
        out_specs=(P(None, "row"), P("row", "col")),
        check_vma=False,
    )
```

```python
import functools

import jax
import jax.numpy as jnp
from jax import lax
from jax.experimental import pallas as pl
from jax.experimental.pallas import tpu as pltpu
from jax.sharding import PartitionSpec as P

MESH = pl.DeviceIdType.MESH
NT = (((1,), (1,)), ((), ()))
SIDE = 4
PIECES = SIDE * SIDE
CHUNK = 256
STORES = 8
FIRST = 4


def remote(src, dst, send, recv, row, col):
    return pltpu.make_async_remote_copy(
        src_ref=src, dst_ref=dst, send_sem=send, recv_sem=recv,
        device_id=(row, col), device_id_type=MESH,
    )


def kernel(
    panel, rhs, inverse, work, solved,
    own, other, mine, cross, made, before, inv,
    panel_send, panel_recv, scatter_send, scatter_recv, before_send, before_recv,
    x_send, x_recv, y_send, y_recv, z_send, z_recv, core_send, core_recv,
    load_sem,
):
    block = inv.shape[0]
    rows_dev = own.shape[0]
    chunks = rows_dev // CHUNK
    row = lax.axis_index("row")
    col = lax.axis_index("col")
    core = lax.rem(col, 2)
    x_hi = lax.rem(col // 2, 2)
    piece = col // 4
    y = lax.rem(piece, SIDE)
    z = piece // SIDE
    length = block // PIECES
    plane = length * SIDE
    has_cross = core == row

    def at(z_, y_, x_, core_):
        return ((z_ * SIDE + y_) * 2 + x_) * 2 + core_

    load_own = pltpu.make_async_copy(panel, own, load_sem.at[0])
    load_first = pltpu.make_async_copy(
        rhs.at[:, pl.ds(0, block)], work.at[:, pl.ds(0, block)], load_sem.at[1]
    )
    load_rest = pltpu.make_async_copy(
        rhs.at[:, pl.ds(block, rows_dev - block)],
        work.at[:, pl.ds(block, rows_dev - block)],
        load_sem.at[2],
    )
    load_inv = pltpu.make_async_copy(inverse.at[core], inv, load_sem.at[3])
    load_first.start()

    @pl.when(col < 2)
    def _():
        load_inv.start()

    barrier = pltpu.get_barrier_semaphore()

    def greet(row_, col_):
        pl.semaphore_signal(barrier, inc=1, device_id=(row_, col_), device_id_type=MESH)

    greet(1 - row, col)
    greet(row, at(z, y, x_hi, 1 - core))
    greet(row, at(z, y, 1 - x_hi, core))
    greet(1 - row, at(z, y, 1 - x_hi, core))
    for d in range(1, SIDE):
        greet(row, at(z, lax.rem(y + d, SIDE), x_hi, core))
        greet(row, at(lax.rem(z + d, SIDE), y, x_hi, core))

    @pl.when(col < 2)
    def _():
        @pl.loop(1, PIECES)
        def _(p):
            greet(row, p * 4 + core)

    @pl.when((x_hi == 0) & (piece > 0))
    def _():
        greet(row, core)

    pl.semaphore_wait(
        barrier,
        10 + jnp.where(col < 2, PIECES - 1, 0) + jnp.where((x_hi == 0) & (piece > 0), 1, 0),
    )

    def panel_copy(j):
        part = pl.ds(pl.multiple_of(j * CHUNK, CHUNK), CHUNK)
        return remote(
            panel.at[part], other.at[part], panel_send.at[j], panel_recv.at[j], 1 - row, col
        )

    own_dropped = (col < 2) & (row >= col)
    other_dropped = (col < 2) & (1 - row >= col)
    top = block // CHUNK

    def top_copies(act):
        for j in range(top):
            act(panel_copy(j))

    @pl.when(~own_dropped)
    def _():
        top_copies(lambda copy: copy.start())

    @pl.loop(top, FIRST)
    def _(j):
        panel_copy(j).start()

    load_own.start()
    load_rest.start()
    load_first.wait()
    load_own.wait()
    load_rest.wait()

    before_copy = remote(made, before, before_send, before_recv, row, 1)

    def scatter_copy(p):
        part = pl.ds(pl.multiple_of(p * length, length), length)
        return remote(
            made.at[part], mine.at[core, part], scatter_send.at[p], scatter_recv, row, p * 4 + core
        )

    def solve(factor):
        @pl.loop(0, 4)
        def _(i):
            tall = block // 4
            part = pl.ds(pl.multiple_of(i * tall, tall), tall)
            rest = work[part, :block]
            if factor is not None:
                rest = rest - lax.dot_general(
                    before[part, :], factor[:block, :], NT, preferred_element_type=jnp.float32
                )
            high = rest.astype(jnp.bfloat16)
            rest = rest - high.astype(jnp.float32)
            middle = rest.astype(jnp.bfloat16)
            low = (rest - middle.astype(jnp.float32)).astype(jnp.bfloat16)
            total = lax.dot_general(low, inv[...], NT, preferred_element_type=jnp.float32)
            total += lax.dot_general(middle, inv[...], NT, preferred_element_type=jnp.float32)
            total += lax.dot_general(high, inv[...], NT, preferred_element_type=jnp.float32)
            made[part, :] = total.astype(jnp.bfloat16)

    @pl.when(col < 2)
    def _():
        load_inv.wait()

        @pl.when(col == 0)
        def _():
            solve(None)
            before_copy.start()

        @pl.when(col == 1)
        def _():
            before_copy.wait_recv()

            @pl.when(row == 0)
            def _():
                solve(own)

            @pl.when(row == 1)
            def _():
                top_copies(lambda copy: copy.wait_recv())
                solve(other)

        @pl.loop(1, PIECES)
        def _(p):
            scatter_copy(p).start()

        mine[core, :length, :] = made[:length, :]

    def spot(p, count=1):
        return pl.ds(pl.multiple_of(p * length, length), length * count)

    here = spot(piece)
    x_across = remote(
        mine.at[core, here], mine.at[core, here], x_send.at[0], x_recv.at[0], row, at(z, y, 1, core)
    )
    x_cross = [
        remote(
            mine.at[core, here], cross.at[here], x_send.at[1 + i], x_recv.at[1],
            1 - row, at(z, y, i, core),
        )
        for i in range(2)
    ]

    @pl.when(x_hi == 0)
    def _():
        @pl.when(piece > 0)
        def _():
            scatter_copy(piece).wait_recv()

        x_across.start()

        @pl.when(~has_cross)
        def _():
            for copy in x_cross:
                copy.start()

    @pl.loop(FIRST, chunks)
    def _(j):
        panel_copy(j).start()

    @pl.when(x_hi == 1)
    def _():
        x_across.wait_recv()

    def y_copy(which, buffer, d, p):
        return remote(
            buffer.at[spot(p)], buffer.at[spot(p)], y_send.at[which, d - 1], y_recv.at[which, d - 1],
            row, at(z, lax.rem(y + d, SIDE), x_hi, core),
        )

    def z_copy(which, buffer, d, p):
        return remote(
            buffer.at[spot(p, SIDE)], buffer.at[spot(p, SIDE)],
            z_send.at[which, d - 1], z_recv.at[which, d - 1],
            row, at(lax.rem(z + d, SIDE), y, x_hi, core),
        )

    own_half = mine.at[core]
    for d in range(1, SIDE):
        y_copy(0, own_half, d, piece).start()

    @pl.when(has_cross)
    def _():
        x_cross[0].wait_recv()
        for d in range(1, SIDE):
            y_copy(1, cross, d, piece).start()

    def y_from(d):
        return z * SIDE + lax.rem(y + SIDE - d, SIDE)

    def z_from(d):
        return lax.rem(z + SIDE - d, SIDE) * SIDE

    for d in range(1, SIDE):
        y_copy(0, own_half, d, y_from(d)).wait_recv()
    for d in range(1, SIDE):
        z_copy(0, own_half, d, z * SIDE).start()

    @pl.when(has_cross)
    def _():
        for d in range(1, SIDE):
            y_copy(1, cross, d, y_from(d)).wait_recv()
        for d in range(1, SIDE):
            z_copy(1, cross, d, z * SIDE).start()

    buddy = at(z, y, x_hi, 1 - core)
    give = remote(own_half, own_half, core_send.at[0], core_recv.at[0], row, buddy)
    theirs = mine.at[1 - core]
    take = remote(theirs, theirs, core_send.at[0], core_recv.at[0], row, buddy)
    share_cross = remote(cross, cross, core_send.at[1], core_recv.at[1], row, buddy)

    for d in range(1, SIDE):
        z_copy(0, own_half, d, z_from(d)).wait_recv()
    give.start()

    @pl.when(has_cross)
    def _():
        for d in range(1, SIDE):
            z_copy(1, cross, d, z_from(d)).wait_recv()
        share_cross.start()

    take.wait_recv()

    @pl.when(~has_cross)
    def _():
        share_cross.wait_recv()

    solved[pl.ds(pl.multiple_of(row * block, block), block), :] = mine[row]
    solved[pl.ds(pl.multiple_of((1 - row) * block, block), block), :] = cross[...]

    @pl.when(own_dropped)
    def _():
        own[:block, :] = jnp.zeros((block, own.shape[1]), own.dtype)

    @pl.when(other_dropped)
    def _():
        other[:block, :] = jnp.zeros((block, other.shape[1]), other.dtype)

    @pl.when(~other_dropped & ~((col == 1) & (row == 1)))
    def _():
        top_copies(lambda copy: copy.wait_recv())

    def update(j):
        part = pl.ds(pl.multiple_of(j * CHUNK, CHUNK), CHUNK)
        total = lax.dot_general(
            mine[row], own[part, :], NT, preferred_element_type=jnp.float32
        )
        total += lax.dot_general(
            mine[1 - row], other[part, :], NT, preferred_element_type=jnp.float32
        )
        work[:, part] -= total

    @pl.loop(0, top)
    def _(j):
        update(j)

    @pl.loop(top, chunks)
    def _(j):
        panel_copy(j).wait_recv()
        update(j)

    @pl.when(~own_dropped)
    def _():
        top_copies(lambda copy: copy.wait_send())

    @pl.loop(top, chunks)
    def _(j):
        panel_copy(j).wait_send()


    give.wait_send()
    for d in range(1, SIDE):
        y_copy(0, own_half, d, piece).wait_send()
        z_copy(0, own_half, d, z * SIDE).wait_send()

    @pl.when(has_cross)
    def _():
        share_cross.wait_send()
        for d in range(1, SIDE):
            y_copy(1, cross, d, piece).wait_send()
            z_copy(1, cross, d, z * SIDE).wait_send()

    @pl.when(x_hi == 0)
    def _():
        x_across.wait_send()

        @pl.when(~has_cross)
        def _():
            for copy in x_cross:
                copy.wait_send()

    @pl.when(col < 2)
    def _():
        @pl.when(col == 0)
        def _():
            before_copy.wait_send()

        @pl.loop(1, PIECES)
        def _(p):
            scatter_copy(p).wait_send()


def flush(work, made, updated, solved, sem):
    rows = work.shape[0] // STORES
    copies = [pltpu.make_async_copy(made, solved, sem.at[STORES])]
    for i in range(STORES):
        part = pl.ds(i * rows, rows)
        copies.append(pltpu.make_async_copy(work.at[part], updated.at[part], sem.at[i]))
    for copy in copies:
        copy.start()
    for copy in copies:
        copy.wait()


def shards(panel, rhs, inverse):
    rows_dev, width = panel.shape
    half = rhs.shape[0]
    block = inverse.shape[1]
    chunks = rows_dev // CHUNK
    on_chip = pl.BlockSpec(memory_space=pltpu.VMEM)
    dma = pltpu.SemaphoreType.DMA
    in_hbm = pl.BlockSpec(memory_space=pltpu.HBM)
    panel, rhs, inverse = (
        pltpu.with_memory_space_constraint(value, pltpu.HBM) for value in (panel, rhs, inverse)
    )
    work, made = pl.pallas_call(
        kernel,
        out_shape=(
            pltpu.VMEM(rhs.shape, jnp.float32),
            pltpu.VMEM((2 * half, block), jnp.bfloat16),
        ),
        in_specs=[in_hbm] * 3,
        out_specs=(on_chip, on_chip),
        scratch_shapes=[
            pltpu.VMEM((rows_dev, width), jnp.bfloat16),
            pltpu.VMEM((rows_dev, width), jnp.bfloat16),
            pltpu.VMEM((2, half, block), jnp.bfloat16),
            pltpu.VMEM((half, block), jnp.bfloat16),
            pltpu.VMEM((half, block), jnp.bfloat16),
            pltpu.VMEM((half, block), jnp.bfloat16),
            pltpu.VMEM((block, block), jnp.bfloat16),
            dma((chunks,)), dma((chunks,)), dma((PIECES,)), dma, dma, dma,
            dma((3,)), dma((2,)), dma((2, 3)), dma((2, 3)), dma((2, 3)), dma((2, 3)),
            dma((2,)), dma((2,)),
            dma((4,)),
        ],
        compiler_params=pltpu.CompilerParams(
            collective_id=0, has_side_effects=True, vmem_limit_bytes=24 << 20
        ),
        name="window",
    )(panel, rhs, inverse)
    updated, solved = pl.pallas_call(
        flush,
        out_shape=(
            jax.ShapeDtypeStruct(rhs.shape, jnp.float32),
            jax.ShapeDtypeStruct((2 * half, block), jnp.bfloat16),
        ),
        in_specs=[on_chip] * 2,
        out_specs=(in_hbm, in_hbm),
        scratch_shapes=[dma((STORES + 1,))],
        compiler_params=pltpu.CompilerParams(vmem_limit_bytes=16 << 20),
        name="flush",
    )(work, made)
    return solved, updated


def solution(mesh):
    return jax.shard_map(
        shards,
        mesh=mesh,
        in_specs=(P("col", "row"), P("row", "col"), P()),
        out_specs=(P(None, "row"), P("row", "col")),
        check_vma=False,
    )
```

```python
import functools

import jax
import jax.numpy as jnp
from jax import lax
from jax.experimental import pallas as pl
from jax.experimental.pallas import tpu as pltpu
from jax.sharding import PartitionSpec as P


MESH = pl.DeviceIdType.MESH
NT = (((1,), (1,)), ((), ()))
SIDE = 4
PIECES = SIDE * SIDE
CHUNK = 256
PARTS = (512, 768, 768, 768, 256)
EARLY = 2
DMA = pltpu.SemaphoreType.DMA
HBM = pl.BlockSpec(memory_space=pltpu.HBM)
VMEM = pl.BlockSpec(memory_space=pltpu.VMEM)
ANY = pl.BlockSpec(memory_space=pl.ANY)
BUSY = pl.CostEstimate(flops=10**10, bytes_accessed=10**6, transcendentals=0)


def place():
    row = lax.axis_index("row")
    col = lax.axis_index("col")
    piece = col // 4
    return row, col, lax.rem(col, 2), lax.rem(col // 2, 2), piece // SIDE, lax.rem(piece, SIDE)


def at(z, y, x, core):
    return ((z * SIDE + y) * 2 + x) * 2 + core


def remote(src, dst, send, recv, row, col):
    return pltpu.make_async_remote_copy(
        src_ref=src, dst_ref=dst, send_sem=send, recv_sem=recv,
        device_id=(row, col), device_id_type=MESH,
    )


def greet(row, col):
    pl.semaphore_signal(
        pltpu.get_barrier_semaphore(), inc=1, device_id=(row, col), device_id_type=MESH
    )


def rows(i, length):
    return pl.ds(pl.multiple_of(i * length, length), length)


def cut_kernel(panel, after, *refs):
    *parts, sem = refs
    start = panel.shape[0] - sum(part.shape[0] for part in parts)
    copies = []
    for i, part in enumerate(parts):
        copies.append(
            pltpu.make_async_copy(panel.at[pl.ds(start, part.shape[0])], part, sem.at[i])
        )
        start += part.shape[0]
    for copy in copies:
        copy.start()
    for copy in copies:
        copy.wait()


def first_kernel(panel, part, sem):
    copy = pltpu.make_async_copy(panel.at[pl.ds(0, part.shape[0])], part, sem)
    copy.start()
    copy.wait()


def cut(panel, lengths):
    width = panel.shape[1]
    params = pltpu.CompilerParams(vmem_limit_bytes=8 << 20)
    first = pl.pallas_call(
        first_kernel,
        out_shape=pltpu.VMEM((lengths[0], width), panel.dtype),
        in_specs=[HBM],
        out_specs=VMEM,
        scratch_shapes=[DMA],
        compiler_params=params,
        name="cut_first",
    )(panel)
    others = pl.pallas_call(
        cut_kernel,
        out_shape=tuple(pltpu.VMEM((length, width), panel.dtype) for length in lengths[1:]),
        in_specs=[HBM, ANY],
        out_specs=(VMEM,) * len(lengths[1:]),
        scratch_shapes=[DMA((len(lengths) - 1,))],
        compiler_params=params,
        name="cut_others",
    )(panel, first)
    return [first, *others]


def solve(value, before, below, inv, made):
    tall = made.shape[0] // 4

    @pl.loop(0, 4)
    def _(i):
        part = rows(i, tall)
        rest = value[part, : made.shape[1]]
        if below is not None:
            rest = rest - lax.dot_general(
                before[part, :], below[...], NT, preferred_element_type=jnp.float32
            )
        high = rest.astype(jnp.bfloat16)
        rest = rest - high.astype(jnp.float32)
        middle = rest.astype(jnp.bfloat16)
        low = (rest - middle.astype(jnp.float32)).astype(jnp.bfloat16)
        total = lax.dot_general(low, inv[...], NT, preferred_element_type=jnp.float32)
        total += lax.dot_general(middle, inv[...], NT, preferred_element_type=jnp.float32)
        total += lax.dot_general(high, inv[...], NT, preferred_element_type=jnp.float32)
        made[part, :] = total.astype(jnp.bfloat16)


def piece_rows(h, z, y, half):
    length = half // (2 * PIECES)
    index = z * SIDE + y if h == 0 else y * SIDE + z
    return pl.ds(pl.multiple_of(h * (half // 2) + index * length, length), length)


def scatter_copy(h, p, made, land, send, recv, row, core):
    length = land.shape[0] // 2
    source = made.at[piece_rows(h, p // SIDE, lax.rem(p, SIDE), made.shape[0])]
    return remote(
        source, land.at[pl.ds(h * length, length)], send.at[h, p], recv.at[h], row, p * 4 + core
    )


def keep_own(made, piece_out):
    length = piece_out.shape[0] // 2
    for h in range(2):
        piece_out[h * length : (h + 1) * length, :] = made[piece_rows(h, 0, 0, made.shape[0]), :]


def early_kernel(
    rhs, panel, inverse, after, held, piece_out, before,
    factor, inv, made, land, load_sem, scatter_send, scatter_recv, before_send, before_recv,
):
    row, col, core, x_hi, _, _ = place()
    piece = col // 4
    block = inv.shape[0]
    late = (row == 1) & (core == 1)

    load_value = pltpu.make_async_copy(
        rhs.at[:, pl.ds(0, block)], held.at[:, pl.ds(0, block)], load_sem.at[0]
    )
    others = pl.ds(block, rhs.shape[1] - block)
    load_others = pltpu.make_async_copy(rhs.at[:, others], held.at[:, others], load_sem.at[1])
    load_value.start()
    before_copy = remote(made, before, before_send, before_recv, row, 1)

    @pl.when(col < 2)
    def _():
        load_inv = pltpu.make_async_copy(inverse.at[core], inv, load_sem.at[2])
        load_factor = pltpu.make_async_copy(panel.at[pl.ds(0, block)], factor, load_sem.at[3])
        load_inv.start()
        load_factor.start()
        greet(row, 1 - core)

        @pl.when(~late)
        def _():
            @pl.loop(1, PIECES)
            def _(p):
                greet(row, p * 4 + core)

        load_others.start()
        pl.semaphore_wait(
            pltpu.get_barrier_semaphore(), 1 + jnp.where(late, 0, PIECES - 1)
        )
        load_value.wait()
        load_inv.wait()
        load_factor.wait()

        @pl.when(col == 0)
        def _():
            solve(held, None, None, inv, made)
            before_copy.start()

        @pl.when(col == 1)
        def _():
            before_copy.wait_recv()

            @pl.when(row == 0)
            def _():
                solve(held, before, factor, inv, made)

        @pl.when(~late)
        def _():
            @pl.loop(1, PIECES)
            def _(p):
                for h in range(2):
                    scatter_copy(h, p, made, land, scatter_send, scatter_recv, row, core).start()

            keep_own(made, piece_out)

        @pl.when(col == 0)
        def _():
            before_copy.wait_send()

        @pl.when(~late)
        def _():
            @pl.loop(1, PIECES)
            def _(p):
                for h in range(2):
                    scatter_copy(
                        h, p, made, land, scatter_send, scatter_recv, row, core
                    ).wait_send()

    @pl.when(col >= 2)
    def _():
        load_others.start()
        load_value.wait()

    @pl.when((x_hi == 0) & (piece > 0) & ~late)
    def _():
        greet(row, core)
        pl.semaphore_wait(pltpu.get_barrier_semaphore(), 1)
        for h in range(2):
            scatter_copy(
                h, piece, made, land, scatter_send, scatter_recv, row, core
            ).wait_recv()
        piece_out[...] = land[...]

    load_others.wait()


def solve_early(rhs, panel, inverse, after):
    half, block = rhs.shape[0], inverse.shape[1]
    length = half // PIECES
    return pl.pallas_call(
        early_kernel,
        out_shape=(
            pltpu.VMEM(rhs.shape, rhs.dtype),
            pltpu.VMEM((length, block), jnp.bfloat16),
            pltpu.VMEM((half, block), jnp.bfloat16),
        ),
        in_specs=[HBM] * 3 + [ANY],
        out_specs=(VMEM,) * 3,
        scratch_shapes=[
            pltpu.VMEM((block, block), jnp.bfloat16),
            pltpu.VMEM((block, block), jnp.bfloat16),
            pltpu.VMEM((half, block), jnp.bfloat16),
            pltpu.VMEM((length, block), jnp.bfloat16),
            DMA((4,)), DMA((2, PIECES)), DMA((2,)), DMA, DMA,
        ],
        compiler_params=pltpu.CompilerParams(
            collective_id=0, has_side_effects=True, vmem_limit_bytes=20 << 20
        ),
        cost_estimate=BUSY,
        name="early",
    )(rhs, panel, inverse, after)


def late_kernel(
    inverse, held, piece_in, before, first, piece_out,
    inv, made, land, load_sem, scatter_send, scatter_recv,
):
    row, col, core, x_hi, _, _ = place()
    piece = col // 4
    late = (row == 1) & (core == 1) & (x_hi == 0)

    @pl.when(~late)
    def _():
        piece_out[...] = piece_in[...]

    @pl.when(late & (piece == 0))
    def _():
        load_inv = pltpu.make_async_copy(inverse.at[1], inv, load_sem)
        load_inv.start()

        @pl.loop(1, PIECES)
        def _(p):
            greet(row, p * 4 + core)

        load_inv.wait()
        solve(held, before, first, inv, made)
        pl.semaphore_wait(pltpu.get_barrier_semaphore(), PIECES - 1)

        @pl.loop(1, PIECES)
        def _(p):
            for h in range(2):
                scatter_copy(h, p, made, land, scatter_send, scatter_recv, row, core).start()

        keep_own(made, piece_out)

        @pl.loop(1, PIECES)
        def _(p):
            for h in range(2):
                scatter_copy(h, p, made, land, scatter_send, scatter_recv, row, core).wait_send()

    @pl.when(late & (piece > 0))
    def _():
        greet(row, core)
        pl.semaphore_wait(pltpu.get_barrier_semaphore(), 1)
        for h in range(2):
            scatter_copy(h, piece, made, land, scatter_send, scatter_recv, row, core).wait_recv()
        piece_out[...] = land[...]


def solve_late(inverse, held, piece, before, first):
    half, block = before.shape
    return pl.pallas_call(
        late_kernel,
        out_shape=pltpu.VMEM(piece.shape, piece.dtype),
        in_specs=[HBM] + [VMEM] * 4,
        out_specs=VMEM,
        scratch_shapes=[
            pltpu.VMEM((block, block), jnp.bfloat16),
            pltpu.VMEM((half, block), jnp.bfloat16),
            pltpu.VMEM(piece.shape, jnp.bfloat16),
            DMA, DMA((2, PIECES)), DMA((2,)),
        ],
        compiler_params=pltpu.CompilerParams(
            collective_id=1, has_side_effects=True, vmem_limit_bytes=20 << 20
        ),
        cost_estimate=BUSY,
        name="late",
    )(inverse, held, piece, before, first)


def gather_kernel(
    own_piece, taken, full, rest,
    mine, cross, x_send, x_recv, send_sem, recv_sem, core_send, core_recv,
):
    row, _, core, x_hi, z, y = place()
    half = cross.shape[0]
    length = own_piece.shape[0] // 2
    has_cross = core == row
    steps = range(1, SIDE)

    @pl.when(x_hi == 0)
    def _():
        for h in range(2):
            here = slice(h * length, (h + 1) * length)
            mine[core, piece_rows(h, z, y, half), :] = own_piece[here, :]

            @pl.when(has_cross)
            def _():
                cross[piece_rows(h, z, y, half), :] = taken[here, :]

    side = at(z, y, 1 - x_hi, core)
    greet(1 - row, side)
    greet(row, at(z, y, x_hi, 1 - core))
    for d in steps:
        greet(row, at(z, lax.rem(y + d, SIDE), x_hi, core))
        greet(row, at(lax.rem(z + d, SIDE), y, x_hi, core))
    pl.semaphore_wait(pltpu.get_barrier_semaphore(), 8)

    def x_copy(which, h):
        here = pl.ds(h * length, length)
        to = piece_rows(h, z, y, half)
        return remote(
            (own_piece if which else taken).at[here],
            cross.at[to] if which else mine.at[core, to],
            x_send.at[which, h], x_recv.at[which, h], 1 - row, side,
        )

    @pl.when(x_hi == 0)
    def _():
        for h in range(2):
            x_copy(0, h).start()

        @pl.when(~has_cross)
        def _():
            for h in range(2):
                x_copy(1, h).start()

    @pl.when(x_hi == 1)
    def _():
        for h in range(2):
            x_copy(0, h).wait_recv()

        @pl.when(has_cross)
        def _():
            for h in range(2):
                x_copy(1, h).wait_recv()

    def copy(which, h, stage, d, back=False):
        buffer = cross if which else mine.at[core]
        along_y = (h == 0) == (stage == 0)
        turn = SIDE - d if back else d
        y_, z_ = (lax.rem(y + turn, SIDE), z) if along_y else (y, lax.rem(z + turn, SIDE))
        from_y, from_z = (y_, z_) if back else (y, z)
        if stage == 0:
            part = piece_rows(h, from_z, from_y, half)
        else:
            group = from_z if h == 0 else from_y
            part = pl.ds(
                pl.multiple_of(h * (half // 2) + group * (half // 8), half // 8), half // 8
            )
        y_to, z_to = (lax.rem(y + d, SIDE), z) if along_y else (y, lax.rem(z + d, SIDE))
        return remote(
            buffer.at[part], buffer.at[part],
            send_sem.at[which, h, stage, d - 1], recv_sem.at[which, h, stage, d - 1],
            row, at(z_to, y_to, x_hi, core),
        )

    def start(which, stage, h):
        for d in steps:
            copy(which, h, stage, d).start()

    def arrive(which, stage, h):
        for d in steps:
            copy(which, h, stage, d, True).wait_recv()

    for h in range(2):
        start(0, 0, h)

    @pl.when(has_cross)
    def _():
        for h in range(2):
            start(1, 0, h)

    for h in range(2):
        arrive(0, 0, h)
        start(0, 1, h)

    @pl.when(has_cross)
    def _():
        for h in range(2):
            arrive(1, 0, h)
            start(1, 1, h)

    buddy = at(z, y, x_hi, 1 - core)

    def share(which, h, take=False):
        part = pl.ds(h * (half // 2), half // 2)
        buffer = cross if which else mine.at[1 - core if take else core]
        return remote(
            buffer.at[part], buffer.at[part], core_send.at[which, h], core_recv.at[which, h],
            row, buddy,
        )

    for h in range(2):
        arrive(0, 1, h)
        share(0, h).start()

    @pl.when(has_cross)
    def _():
        for h in range(2):
            arrive(1, 1, h)
            share(1, h).start()

    for h in range(2):
        share(0, h, True).wait_recv()

    @pl.when(~has_cross)
    def _():
        for h in range(2):
            share(1, h, True).wait_recv()

    full[rows(row, half), :] = mine[row]
    full[rows(1 - row, half), :] = cross[...]
    rest[...] = mine[1 - row]

    def sent(which):
        for h in range(2):
            share(which, h).wait_send()
            for stage in range(2):
                for d in steps:
                    copy(which, h, stage, d).wait_send()

    sent(0)

    @pl.when(has_cross)
    def _():
        sent(1)

    @pl.when(x_hi == 0)
    def _():
        for h in range(2):
            x_copy(0, h).wait_send()

        @pl.when(~has_cross)
        def _():
            for h in range(2):
                x_copy(1, h).wait_send()


def gather_pieces(piece, taken):
    length, block = piece.shape
    half = length * PIECES
    return pl.pallas_call(
        gather_kernel,
        out_shape=(
            pltpu.VMEM((2 * half, block), jnp.bfloat16),
            pltpu.VMEM((half, block), jnp.bfloat16),
        ),
        in_specs=[VMEM] * 2,
        out_specs=(VMEM, VMEM),
        scratch_shapes=[
            pltpu.VMEM((2, half, block), jnp.bfloat16),
            pltpu.VMEM((half, block), jnp.bfloat16),
            DMA((2, 2)), DMA((2, 2)), DMA((2, 2, 2, 3)), DMA((2, 2, 2, 3)), DMA((2, 2)), DMA((2, 2)),
        ],
        compiler_params=pltpu.CompilerParams(
            collective_id=2, has_side_effects=True, vmem_limit_bytes=12 << 20
        ),
        cost_estimate=BUSY,
        name="gather",
    )(piece, taken)


def begin_kernel(held, full, rest, *refs, count, early):
    owns, parts = refs[:count], refs[count : count + early]
    updated, solved, ahead, work, store_sem = refs[count + early :]
    row, col = lax.axis_index("row"), lax.axis_index("col")
    block = rest.shape[0]
    ready = work.shape[1]

    put_solved = pltpu.make_async_copy(full, solved, store_sem.at[0])
    put_solved.start()

    def store(j):
        part = rows(j, CHUNK)
        return pltpu.make_async_copy(work.at[:, part], updated.at[:, part], store_sem.at[1 + j])

    def step(first, i, mine, theirs, mask):
        here = rows(i, CHUNK)
        own = mine[here, :]
        if mask:
            own = jnp.where((col < 2) & (row >= col), jnp.zeros_like(own), own)
        total = lax.dot_general(
            full[rows(row, block), :], own, NT, preferred_element_type=jnp.float32
        )
        column = rows(first + i, CHUNK)
        if theirs is None:
            ahead[:, rows(first + i - ready // CHUNK, CHUNK)] = held[:, column] - total
            return
        other = theirs[here, :]
        if mask:
            other = jnp.where((col < 2) & (1 - row >= col), jnp.zeros_like(other), other)
        total += lax.dot_general(rest[...], other, NT, preferred_element_type=jnp.float32)
        work[:, column] = held[:, column] - total
        store(first + i).start()

    first = 0
    for index, mine in enumerate(owns):
        theirs = parts[index] if index < early else None
        here = mine.shape[0] // CHUNK
        top = min(here, max(0, block // CHUNK - first))
        for low, high, mask in ((0, top, True), (top, here, False)):
            if high > low:
                pl.loop(low, high)(
                    functools.partial(
                        lambda i, first, mine, theirs, mask: step(first, i, mine, theirs, mask),
                        first=first, mine=mine, theirs=theirs, mask=mask,
                    )
                )
        first += here

    put_solved.wait()

    @pl.loop(0, ready // CHUNK)
    def _(j):
        store(j).wait()


def begin(held, full, rest, owns, parts):
    half, rows_dev = held.shape
    ready = sum(part.shape[0] for part in parts)
    return pl.pallas_call(
        functools.partial(begin_kernel, count=len(owns), early=len(parts)),
        out_shape=(
            pltpu.HBM(held.shape, jnp.float32),
            pltpu.HBM(full.shape, full.dtype),
            pltpu.VMEM((half, rows_dev - ready), jnp.float32),
        ),
        in_specs=[VMEM] * (3 + len(owns) + len(parts)),
        out_specs=(HBM, HBM, VMEM),
        scratch_shapes=[
            pltpu.VMEM((half, ready), jnp.float32),
            DMA((1 + ready // CHUNK,)),
        ],
        compiler_params=pltpu.CompilerParams(vmem_limit_bytes=32 << 20),
        cost_estimate=BUSY,
        name="begin",
    )(held, full, rest, *owns, *parts)


def finish_kernel(start, offset, held, ahead, part, rest, updated, work, store_sem):
    length = part.shape[0]
    stores = []
    for j in range(length // CHUNK):
        here = pl.ds(j * CHUNK, CHUNK)
        total = lax.dot_general(
            rest[...], part[here, :], NT, preferred_element_type=jnp.float32
        )
        work[:, here] = ahead[:, pl.ds(offset + j * CHUNK, CHUNK)] - total
        stores.append(
            pltpu.make_async_copy(
                work.at[:, here], updated.at[:, pl.ds(start + j * CHUNK, CHUNK)], store_sem.at[j]
            )
        )
        stores[-1].start()
    for copy in stores:
        copy.wait()


def finish(updated, ahead, part, rest, start, offset):
    length = part.shape[0]
    return pl.pallas_call(
        functools.partial(finish_kernel, start, offset),
        out_shape=pltpu.HBM(updated.shape, updated.dtype),
        in_specs=[HBM, VMEM, VMEM, VMEM],
        out_specs=HBM,
        scratch_shapes=[
            pltpu.VMEM((ahead.shape[0], length), jnp.float32),
            DMA((length // CHUNK,)),
        ],
        input_output_aliases={0: 0},
        compiler_params=pltpu.CompilerParams(vmem_limit_bytes=12 << 20),
        cost_estimate=pl.CostEstimate(flops=10**9, bytes_accessed=10**6, transcendentals=0),
    )(updated, ahead, part, rest)


def swap(value):
    taken = lax.ppermute(value, "row", [(0, 1), (1, 0)])
    return pltpu.with_memory_space_constraint(taken, pltpu.VMEM)


def shards(panel, rhs, inverse):
    panel, rhs, inverse = (
        pltpu.with_memory_space_constraint(value, pltpu.HBM) for value in (panel, rhs, inverse)
    )
    count = len(PARTS)
    starts = [sum(PARTS[:i]) for i in range(count)]
    sent = cut(panel, PARTS)
    arrived = [swap(sent[i]) for i in range(count)]
    held, piece, before = solve_early(rhs, panel, inverse, sent[1])
    piece = solve_late(inverse, held, piece, before, arrived[0])
    col_count = lax.axis_size("col")
    pairs = [
        (row * col_count + col + core, (1 - row) * col_count + col + core)
        for row in range(2) for col in range(0, col_count, 4) for core in range(2)
    ]
    taken = lax.ppermute(piece, ("row", "col"), pairs)
    full, rest = gather_pieces(piece, taken)
    updated, solved, ahead = begin(held, full, rest, sent, arrived[:EARLY])
    for i in range(EARLY, count):
        updated = finish(updated, ahead, arrived[i], rest, starts[i], starts[i] - starts[EARLY])
    return solved, updated


def solution(mesh):
    return jax.shard_map(
        shards,
        mesh=mesh,
        in_specs=(P("col", "row"), P("row", "col"), P()),
        out_specs=(P(None, "row"), P("row", "col")),
        check_vma=False,
    )
```

```python
import functools

import jax
import jax.numpy as jnp
from jax import lax
from jax.experimental import pallas as pl
from jax.experimental.pallas import tpu as pltpu
from jax.sharding import PartitionSpec as P


MESH = pl.DeviceIdType.MESH
NT = (((1,), (1,)), ((), ()))
SIDE = 4
PIECES = SIDE * SIDE
PARTS = (512, 768, 768, 896, 128)
EARLY = 2
DMA = pltpu.SemaphoreType.DMA
HBM = pl.BlockSpec(memory_space=pltpu.HBM)
VMEM = pl.BlockSpec(memory_space=pltpu.VMEM)
ANY = pl.BlockSpec(memory_space=pl.ANY)
BUSY = pl.CostEstimate(flops=10**10, bytes_accessed=10**6, transcendentals=0)


def place():
    row = lax.axis_index("row")
    col = lax.axis_index("col")
    piece = col // 4
    return row, col, lax.rem(col, 2), lax.rem(col // 2, 2), piece // SIDE, lax.rem(piece, SIDE)


def at(z, y, x, core):
    return ((z * SIDE + y) * 2 + x) * 2 + core


def remote(src, dst, send, recv, row, col):
    return pltpu.make_async_remote_copy(
        src_ref=src, dst_ref=dst, send_sem=send, recv_sem=recv,
        device_id=(row, col), device_id_type=MESH,
    )


def greet(row, col):
    pl.semaphore_signal(
        pltpu.get_barrier_semaphore(), inc=1, device_id=(row, col), device_id_type=MESH
    )


def rows(i, length):
    return pl.ds(pl.multiple_of(i * length, length), length)


def cut_kernel(panel, after, *refs):
    *parts, sem = refs
    start = panel.shape[0] - sum(part.shape[0] for part in parts)
    copies = []
    for i, part in enumerate(parts):
        copies.append(
            pltpu.make_async_copy(panel.at[pl.ds(start, part.shape[0])], part, sem.at[i])
        )
        start += part.shape[0]
    for copy in copies:
        copy.start()
    for copy in copies:
        copy.wait()


def lead_kernel(panel, own, got, load_sem, send_sem, recv_sem):
    row, col, core, _, _, _ = place()
    load = pltpu.make_async_copy(panel.at[pl.ds(0, own.shape[0])], own, load_sem)
    load.start()

    @pl.when(core == 1)
    def _():
        copy = remote(own, got, send_sem, recv_sem, 1 - row, col)
        greet(1 - row, col)
        pl.semaphore_wait(pltpu.get_barrier_semaphore(), 1)
        load.wait()
        copy.start()
        copy.wait()

    @pl.when(core == 0)
    def _():
        load.wait()


def lead(panel, length):
    part = pltpu.VMEM((length, panel.shape[1]), panel.dtype)
    return pl.pallas_call(
        lead_kernel,
        out_shape=(part, part),
        in_specs=[HBM],
        out_specs=(VMEM, VMEM),
        scratch_shapes=[DMA, DMA, DMA],
        compiler_params=pltpu.CompilerParams(
            collective_id=1, has_side_effects=True, vmem_limit_bytes=8 << 20
        ),
        name="lead",
    )(panel)


def cut(panel, lengths, first):
    width = panel.shape[1]
    return pl.pallas_call(
        cut_kernel,
        out_shape=tuple(pltpu.VMEM((length, width), panel.dtype) for length in lengths),
        in_specs=[HBM, ANY],
        out_specs=(VMEM,) * len(lengths),
        scratch_shapes=[DMA((len(lengths),))],
        compiler_params=pltpu.CompilerParams(vmem_limit_bytes=8 << 20),
        name="cut",
    )(panel, first)


def solve(value, before, below, inv, made):
    tall = made.shape[0] // 4

    @pl.loop(0, 4)
    def _(i):
        part = rows(i, tall)
        rest = value[part, : made.shape[1]]
        if below is not None:
            rest = rest - lax.dot_general(
                before[part, :], below[...], NT, preferred_element_type=jnp.float32
            )
        high = rest.astype(jnp.bfloat16)
        rest = rest - high.astype(jnp.float32)
        middle = rest.astype(jnp.bfloat16)
        low = (rest - middle.astype(jnp.float32)).astype(jnp.bfloat16)
        total = lax.dot_general(low, inv[...], NT, preferred_element_type=jnp.float32)
        total += lax.dot_general(middle, inv[...], NT, preferred_element_type=jnp.float32)
        total += lax.dot_general(high, inv[...], NT, preferred_element_type=jnp.float32)
        made[part, :] = total.astype(jnp.bfloat16)


def piece_rows(h, z, y, half):
    length = half // (2 * PIECES)
    index = z * SIDE + y if h == 0 else y * SIDE + z
    return pl.ds(pl.multiple_of(h * (half // 2) + index * length, length), length)


def scatter_copy(h, p, made, land, send, recv, row, core):
    source = made.at[piece_rows(h, p // SIDE, lax.rem(p, SIDE), made.shape[0])]
    to_row = row if h == 0 else 1 - row
    return remote(source, land, send.at[h, p], recv, to_row, p * 4 + 2 * h + core)


def solve_kernel(
    rhs, inverse, own, got, after, held, piece_out,
    inv, made, before, land, load_sem, scatter_send, scatter_recv, before_send, before_recv,
):
    row, col, core, x_hi, _, _ = place()
    piece = col // 4
    block = inv.shape[0]
    load_value = pltpu.make_async_copy(
        rhs.at[:, pl.ds(0, block)], held.at[:, pl.ds(0, block)], load_sem.at[0]
    )
    others = pl.ds(block, rhs.shape[1] - block)
    load_others = pltpu.make_async_copy(rhs.at[:, others], held.at[:, others], load_sem.at[1])
    load_value.start()
    before_copy = remote(made, before, before_send, before_recv, row, 1)

    @pl.when(col < 2)
    def _():
        load_inv = pltpu.make_async_copy(inverse.at[core], inv, load_sem.at[2])
        load_inv.start()
        load_others.start()
        greet(row, 1 - core)

        @pl.loop(1, PIECES)
        def _(p):
            greet(row, p * 4 + core)

        @pl.loop(0, PIECES)
        def _(p):
            greet(1 - row, p * 4 + 2 + core)

        load_value.wait()
        load_inv.wait()

        @pl.when(col == 0)
        def _():
            solve(held, None, None, inv, made)

        pl.semaphore_wait(pltpu.get_barrier_semaphore(), 2 * PIECES)

        @pl.when(col == 0)
        def _():
            before_copy.start()

        @pl.when(col == 1)
        def _():
            before_copy.wait_recv()

            @pl.when(row == 0)
            def _():
                solve(held, before, own, inv, made)

            @pl.when(row == 1)
            def _():
                solve(held, before, got, inv, made)

        def scattered(act):
            @pl.loop(1, PIECES)
            def _(p):
                act(scatter_copy(0, p, made, land, scatter_send, scatter_recv, row, core))

            @pl.loop(0, PIECES)
            def _(p):
                act(scatter_copy(1, p, made, land, scatter_send, scatter_recv, row, core))

        scattered(lambda copy: copy.start())
        piece_out[...] = made[piece_rows(0, 0, 0, made.shape[0]), :]

        @pl.when(col == 0)
        def _():
            before_copy.wait_send()

        scattered(lambda copy: copy.wait_send())

    @pl.when(col >= 2)
    def _():
        load_others.start()
        load_value.wait()
        source_row = jnp.where(x_hi == 0, row, 1 - row)
        greet(source_row, core)
        pl.semaphore_wait(pltpu.get_barrier_semaphore(), 1)
        scatter_copy(0, piece, made, land, scatter_send, scatter_recv, row, core).wait_recv()
        piece_out[...] = land[...]

    load_others.wait()


def solve_pieces(rhs, inverse, own, got, after):
    half, block = rhs.shape[0], inverse.shape[1]
    length = half // (2 * PIECES)
    return pl.pallas_call(
        solve_kernel,
        out_shape=(
            pltpu.VMEM(rhs.shape, rhs.dtype),
            pltpu.VMEM((length, block), jnp.bfloat16),
        ),
        in_specs=[HBM] * 2 + [VMEM] * 2 + [ANY],
        out_specs=(VMEM, VMEM),
        scratch_shapes=[
            pltpu.VMEM((block, block), jnp.bfloat16),
            pltpu.VMEM((half, block), jnp.bfloat16),
            pltpu.VMEM((half, block), jnp.bfloat16),
            pltpu.VMEM((length, block), jnp.bfloat16),
            DMA((3,)), DMA((2, PIECES)), DMA, DMA, DMA,
        ],
        compiler_params=pltpu.CompilerParams(
            collective_id=0, has_side_effects=True, vmem_limit_bytes=20 << 20
        ),
        cost_estimate=BUSY,
        name="solve",
    )(rhs, inverse, own, got, after)


def gather_kernel(
    own_piece, taken, full, rest,
    mine, cross, x_send, x_recv, send_sem, recv_sem, core_send, core_recv,
):
    row, _, core, x_hi, z, y = place()
    half = cross.shape[0]
    has_cross = core == row
    steps = range(1, SIDE)

    for h, (kept, crossed) in enumerate(((own_piece, taken), (taken, own_piece))):
        @pl.when(x_hi == h)
        def _():
            here = piece_rows(h, z, y, half)
            mine[core, here, :] = kept[...]

            @pl.when(has_cross)
            def _():
                cross[here, :] = crossed[...]

    side = at(z, y, 1 - x_hi, core)
    greet(1 - row, side)
    greet(row, at(z, y, x_hi, 1 - core))
    for d in steps:
        greet(row, at(z, lax.rem(y + d, SIDE), x_hi, core))
        greet(row, at(lax.rem(z + d, SIDE), y, x_hi, core))
    pl.semaphore_wait(pltpu.get_barrier_semaphore(), 8)

    def x_copy(which, h, source):
        to = piece_rows(h, z, y, half)
        return remote(
            source, cross.at[to] if which else mine.at[core, to],
            x_send.at[which], x_recv.at[which], 1 - row, side,
        )

    for h, (kept, crossed) in enumerate(((own_piece, taken), (taken, own_piece))):
        @pl.when(x_hi == h)
        def _():
            x_copy(0, h, crossed).start()

            @pl.when(~has_cross)
            def _():
                x_copy(1, h, kept).start()

    for h in range(2):
        @pl.when(x_hi == 1 - h)
        def _():
            x_copy(0, h, taken).wait_recv()

            @pl.when(has_cross)
            def _():
                x_copy(1, h, taken).wait_recv()

    def copy(which, h, stage, d, back=False):
        buffer = cross if which else mine.at[core]
        along_y = (h == 0) == (stage == 0)
        turn = SIDE - d if back else d
        y_, z_ = (lax.rem(y + turn, SIDE), z) if along_y else (y, lax.rem(z + turn, SIDE))
        from_y, from_z = (y_, z_) if back else (y, z)
        if stage == 0:
            part = piece_rows(h, from_z, from_y, half)
        else:
            group = from_z if h == 0 else from_y
            part = pl.ds(
                pl.multiple_of(h * (half // 2) + group * (half // 8), half // 8), half // 8
            )
        y_to, z_to = (lax.rem(y + d, SIDE), z) if along_y else (y, lax.rem(z + d, SIDE))
        return remote(
            buffer.at[part], buffer.at[part],
            send_sem.at[which, h, stage, d - 1], recv_sem.at[which, h, stage, d - 1],
            row, at(z_to, y_to, x_hi, core),
        )

    def start(which, stage, h):
        for d in steps:
            copy(which, h, stage, d).start()

    def arrive(which, stage, h):
        for d in steps:
            copy(which, h, stage, d, True).wait_recv()

    for h in range(2):
        start(0, 0, h)

    @pl.when(has_cross)
    def _():
        for h in range(2):
            start(1, 0, h)

    for h in range(2):
        arrive(0, 0, h)
        start(0, 1, h)

    @pl.when(has_cross)
    def _():
        for h in range(2):
            arrive(1, 0, h)
            start(1, 1, h)

    buddy = at(z, y, x_hi, 1 - core)

    def share(which, h, take=False):
        part = pl.ds(h * (half // 2), half // 2)
        buffer = cross if which else mine.at[1 - core if take else core]
        return remote(
            buffer.at[part], buffer.at[part], core_send.at[which, h], core_recv.at[which, h],
            row, buddy,
        )

    for h in range(2):
        arrive(0, 1, h)
        share(0, h).start()

    @pl.when(has_cross)
    def _():
        for h in range(2):
            arrive(1, 1, h)
            share(1, h).start()

    for h in range(2):
        share(0, h, True).wait_recv()

    @pl.when(~has_cross)
    def _():
        for h in range(2):
            share(1, h, True).wait_recv()

    full[rows(row, half), :] = mine[row]
    full[rows(1 - row, half), :] = cross[...]
    rest[...] = mine[1 - row]

    def sent(which):
        for h in range(2):
            share(which, h).wait_send()
            for stage in range(2):
                for d in steps:
                    copy(which, h, stage, d).wait_send()

    sent(0)

    @pl.when(has_cross)
    def _():
        sent(1)

    x_copy(0, 0, taken).wait_send()

    @pl.when(~has_cross)
    def _():
        x_copy(1, 0, taken).wait_send()


def gather_pieces(piece, taken):
    length, block = piece.shape
    half = length * 2 * PIECES
    return pl.pallas_call(
        gather_kernel,
        out_shape=(
            pltpu.VMEM((2 * half, block), jnp.bfloat16),
            pltpu.VMEM((half, block), jnp.bfloat16),
        ),
        in_specs=[VMEM] * 2,
        out_specs=(VMEM, VMEM),
        scratch_shapes=[
            pltpu.VMEM((2, half, block), jnp.bfloat16),
            pltpu.VMEM((half, block), jnp.bfloat16),
            DMA((2,)), DMA((2,)), DMA((2, 2, 2, 3)), DMA((2, 2, 2, 3)), DMA((2, 2)), DMA((2, 2)),
        ],
        compiler_params=pltpu.CompilerParams(
            collective_id=2, has_side_effects=True, vmem_limit_bytes=12 << 20
        ),
        cost_estimate=BUSY,
        name="gather",
    )(piece, taken)


def chunk_of(length):
    return 256 if length % 256 == 0 else 128


def begin_kernel(held, full, rest, *refs, count, early):
    owns, parts, got = refs[:count], refs[count : count + early], refs[count + early]
    updated, solved, ahead, work, store_sem = refs[count + early + 1 :]
    row, col = lax.axis_index("row"), lax.axis_index("col")
    block = rest.shape[0]
    ready = work.shape[1]

    put_solved = pltpu.make_async_copy(full, solved, store_sem.at[0])
    put_solved.start()

    def store(index, start, length):
        part = pl.ds(start, length)
        return pltpu.make_async_copy(
            work.at[:, part], updated.at[:, part], store_sem.at[1 + index]
        )

    def step(i, start, mine, theirs):
        chunk = chunk_of(mine.shape[0])
        here = rows(i, chunk)
        column = pl.ds(pl.multiple_of(start + i * chunk, chunk), chunk)
        own = mine[here, :]
        if start == 0:
            own = jnp.where((col < 2) & (row >= col), jnp.zeros_like(own), own)
        total = lax.dot_general(
            full[rows(row, block), :], own, NT, preferred_element_type=jnp.float32
        )
        if theirs is None:
            ahead[:, pl.ds(pl.multiple_of(start + i * chunk - ready, chunk), chunk)] = (
                held[:, column] - total
            )
            return
        other = theirs[here, :]
        if start == 0:
            other = jnp.where(lax.rem(col, 2) == 1, got[here, :], other)
            other = jnp.where((col < 2) & (1 - row >= col), jnp.zeros_like(other), other)
        total += lax.dot_general(rest[...], other, NT, preferred_element_type=jnp.float32)
        work[:, column] = held[:, column] - total

    start = 0
    stores = []
    for index, mine in enumerate(owns):
        length = mine.shape[0]
        theirs = parts[index] if index < early else None
        pl.loop(0, length // chunk_of(length))(
            functools.partial(step, start=start, mine=mine, theirs=theirs)
        )
        if index < early:
            stores.append(store(index, start, length))
            stores[-1].start()
        start += length

    put_solved.wait()
    for copy in stores:
        copy.wait()


def begin(held, full, rest, owns, parts, got):
    half, rows_dev = held.shape
    ready = sum(part.shape[0] for part in parts)
    return pl.pallas_call(
        functools.partial(begin_kernel, count=len(owns), early=len(parts)),
        out_shape=(
            pltpu.HBM(held.shape, jnp.float32),
            pltpu.HBM(full.shape, full.dtype),
            pltpu.VMEM((half, rows_dev - ready), jnp.float32),
        ),
        in_specs=[VMEM] * (4 + len(owns) + len(parts)),
        out_specs=(HBM, HBM, VMEM),
        scratch_shapes=[
            pltpu.VMEM((half, ready), jnp.float32),
            DMA((1 + len(parts),)),
        ],
        compiler_params=pltpu.CompilerParams(vmem_limit_bytes=32 << 20),
        cost_estimate=BUSY,
        name="begin",
    )(held, full, rest, *owns, *parts, got)


def finish_kernel(start, offset, held, ahead, part, rest, updated, work, store_sem):
    length = part.shape[0]
    chunk = chunk_of(length)
    stores = []
    for j in range(length // chunk):
        here = pl.ds(j * chunk, chunk)
        total = lax.dot_general(
            rest[...], part[here, :], NT, preferred_element_type=jnp.float32
        )
        work[:, here] = ahead[:, pl.ds(offset + j * chunk, chunk)] - total
        stores.append(
            pltpu.make_async_copy(
                work.at[:, here], updated.at[:, pl.ds(start + j * chunk, chunk)], store_sem.at[j]
            )
        )
        stores[-1].start()
    for copy in stores:
        copy.wait()


def finish(updated, ahead, part, rest, start, offset):
    length = part.shape[0]
    return pl.pallas_call(
        functools.partial(finish_kernel, start, offset),
        out_shape=pltpu.HBM(updated.shape, updated.dtype),
        in_specs=[HBM, VMEM, VMEM, VMEM],
        out_specs=HBM,
        scratch_shapes=[
            pltpu.VMEM((ahead.shape[0], length), jnp.float32),
            DMA((length // chunk_of(length),)),
        ],
        input_output_aliases={0: 0},
        compiler_params=pltpu.CompilerParams(vmem_limit_bytes=12 << 20),
        cost_estimate=pl.CostEstimate(flops=10**9, bytes_accessed=10**6, transcendentals=0),
    )(updated, ahead, part, rest)


def swap(value, cores=(0, 1)):
    col_count = lax.axis_size("col")
    pairs = [
        (row * col_count + col, (1 - row) * col_count + col)
        for row in range(2) for col in range(col_count) if col % 2 in cores
    ]
    taken = lax.ppermute(value, ("row", "col"), pairs)
    return pltpu.with_memory_space_constraint(taken, pltpu.VMEM)


def shards(panel, rhs, inverse):
    panel, rhs, inverse = (
        pltpu.with_memory_space_constraint(value, pltpu.HBM) for value in (panel, rhs, inverse)
    )
    count = len(PARTS)
    starts = [sum(PARTS[:i]) for i in range(count)]
    first, got = lead(panel, PARTS[0])
    sent = [first, *cut(panel, PARTS[1:], first)]
    arrived = [swap(sent[i], (0, 1) if i else (0,)) for i in range(count)]
    held, piece = solve_pieces(rhs, inverse, first, got, sent[1])
    taken = swap(piece)
    full, rest = gather_pieces(piece, taken)
    updated, solved, ahead = begin(held, full, rest, sent, arrived[:EARLY], got)
    for i in range(EARLY, count):
        updated = finish(updated, ahead, arrived[i], rest, starts[i], starts[i] - starts[EARLY])
    return solved, updated


def solution(mesh):
    return jax.shard_map(
        shards,
        mesh=mesh,
        in_specs=(P("col", "row"), P("row", "col"), P()),
        out_specs=(P(None, "row"), P("row", "col")),
        check_vma=False,
    )
```

```python
import functools

import jax
import jax.numpy as jnp
from jax import lax
from jax.experimental import pallas as pl
from jax.experimental.pallas import tpu as pltpu
from jax.sharding import PartitionSpec as P


MESH = pl.DeviceIdType.MESH
NT = (((1,), (1,)), ((), ()))
SIDE = 4
PIECES = SIDE * SIDE
PARTS = (512, 768, 768, 640, 256, 128)
EARLY = 2
DMA = pltpu.SemaphoreType.DMA
HBM = pl.BlockSpec(memory_space=pltpu.HBM)
VMEM = pl.BlockSpec(memory_space=pltpu.VMEM)
ANY = pl.BlockSpec(memory_space=pl.ANY)
BUSY = pl.CostEstimate(flops=10**10, bytes_accessed=10**6, transcendentals=0)


def place():
    row = lax.axis_index("row")
    col = lax.axis_index("col")
    piece = col // 4
    return row, col, lax.rem(col, 2), lax.rem(col // 2, 2), piece // SIDE, lax.rem(piece, SIDE)


def at(z, y, x, core):
    return ((z * SIDE + y) * 2 + x) * 2 + core


def remote(src, dst, send, recv, row, col):
    return pltpu.make_async_remote_copy(
        src_ref=src, dst_ref=dst, send_sem=send, recv_sem=recv,
        device_id=(row, col), device_id_type=MESH,
    )


def greet(row, col):
    pl.semaphore_signal(
        pltpu.get_barrier_semaphore(), inc=1, device_id=(row, col), device_id_type=MESH
    )


def rows(i, length):
    return pl.ds(pl.multiple_of(i * length, length), length)


def lead_kernel(panel, *refs):
    *parts, got, load_sem, send_sem, recv_sem = refs
    row, col, core, _, _, _ = place()
    loads = []
    start = 0
    for i, part in enumerate(parts):
        loads.append(
            pltpu.make_async_copy(panel.at[pl.ds(start, part.shape[0])], part, load_sem.at[i])
        )
        start += part.shape[0]
    for load in loads:
        load.start()

    @pl.when(core == 1)
    def _():
        copy = remote(parts[0], got, send_sem, recv_sem, 1 - row, col)
        greet(1 - row, col)
        pl.semaphore_wait(pltpu.get_barrier_semaphore(), 1)
        loads[0].wait()
        copy.start()
        copy.wait()

    @pl.when(core == 0)
    def _():
        loads[0].wait()

    for load in loads[1:]:
        load.wait()


def lead(panel, lengths):
    parts = [pltpu.VMEM((length, panel.shape[1]), panel.dtype) for length in lengths]
    *parts, got = pl.pallas_call(
        lead_kernel,
        out_shape=(*parts, parts[0]),
        in_specs=[HBM],
        out_specs=(VMEM,) * (len(parts) + 1),
        scratch_shapes=[DMA((len(lengths),)), DMA, DMA],
        compiler_params=pltpu.CompilerParams(
            collective_id=1, has_side_effects=True, vmem_limit_bytes=8 << 20
        ),
        name="lead",
    )(panel)
    return parts, got


def solve(value, before, below, inv, made):
    rest = value[:, : made.shape[1]]
    if below is not None:
        rest = rest - lax.dot_general(
            before[...], below[...], NT, preferred_element_type=jnp.float32
        )
    high = rest.astype(jnp.bfloat16)
    rest = rest - high.astype(jnp.float32)
    middle = rest.astype(jnp.bfloat16)
    low = (rest - middle.astype(jnp.float32)).astype(jnp.bfloat16)
    total = lax.dot_general(low, inv[...], NT, preferred_element_type=jnp.float32)
    total += lax.dot_general(middle, inv[...], NT, preferred_element_type=jnp.float32)
    total += lax.dot_general(high, inv[...], NT, preferred_element_type=jnp.float32)
    made[...] = total.astype(jnp.bfloat16)


def piece_rows(h, z, y, half):
    length = half // (2 * PIECES)
    index = z * SIDE + y if h == 0 else y * SIDE + z
    return pl.ds(pl.multiple_of(h * (half // 2) + index * length, length), length)


def scatter_copy(h, p, made, land, send, recv, row, core):
    source = made.at[piece_rows(h, p // SIDE, lax.rem(p, SIDE), made.shape[0])]
    to_row = row if h == 0 else 1 - row
    return remote(source, land, send.at[h, p], recv, to_row, p * 4 + 2 * h + core)


def solve_kernel(
    rhs, inverse, own, got, after, held, piece_out,
    inv, made, before, land, load_sem, scatter_send, scatter_recv, before_send, before_recv,
):
    row, col, core, x_hi, _, _ = place()
    piece = col // 4
    block = inv.shape[0]
    load_value = pltpu.make_async_copy(
        rhs.at[:, pl.ds(0, block)], held.at[:, pl.ds(0, block)], load_sem.at[0]
    )
    others = pl.ds(block, rhs.shape[1] - block)
    load_others = pltpu.make_async_copy(rhs.at[:, others], held.at[:, others], load_sem.at[1])
    load_value.start()
    before_copy = remote(made, before, before_send, before_recv, row, 1)

    @pl.when(col < 2)
    def _():
        load_inv = pltpu.make_async_copy(inverse.at[core], inv, load_sem.at[2])
        load_inv.start()
        load_others.start()
        greet(row, 1 - core)

        @pl.loop(1, PIECES)
        def _(p):
            greet(row, p * 4 + core)

        @pl.loop(0, PIECES)
        def _(p):
            greet(1 - row, p * 4 + 2 + core)

        load_value.wait()
        load_inv.wait()

        @pl.when(col == 0)
        def _():
            solve(held, None, None, inv, made)

        pl.semaphore_wait(pltpu.get_barrier_semaphore(), 2 * PIECES)

        @pl.when(col == 0)
        def _():
            before_copy.start()

        @pl.when(col == 1)
        def _():
            before_copy.wait_recv()

            @pl.when(row == 0)
            def _():
                solve(held, before, own, inv, made)

            @pl.when(row == 1)
            def _():
                solve(held, before, got, inv, made)

        def scattered(act):
            @pl.loop(1, PIECES)
            def _(p):
                act(scatter_copy(0, p, made, land, scatter_send, scatter_recv, row, core))

            @pl.loop(0, PIECES)
            def _(p):
                act(scatter_copy(1, p, made, land, scatter_send, scatter_recv, row, core))

        scattered(lambda copy: copy.start())
        piece_out[...] = made[piece_rows(0, 0, 0, made.shape[0]), :]

        @pl.when(col == 0)
        def _():
            before_copy.wait_send()

        scattered(lambda copy: copy.wait_send())

    @pl.when(col >= 2)
    def _():
        load_others.start()
        load_value.wait()
        source_row = jnp.where(x_hi == 0, row, 1 - row)
        greet(source_row, core)
        pl.semaphore_wait(pltpu.get_barrier_semaphore(), 1)
        scatter_copy(0, piece, made, land, scatter_send, scatter_recv, row, core).wait_recv()
        piece_out[...] = land[...]

    load_others.wait()


def solve_pieces(rhs, inverse, own, got, after):
    half, block = rhs.shape[0], inverse.shape[1]
    length = half // (2 * PIECES)
    return pl.pallas_call(
        solve_kernel,
        out_shape=(
            pltpu.VMEM(rhs.shape, rhs.dtype),
            pltpu.VMEM((length, block), jnp.bfloat16),
        ),
        in_specs=[HBM] * 2 + [VMEM] * 2 + [ANY],
        out_specs=(VMEM, VMEM),
        scratch_shapes=[
            pltpu.VMEM((block, block), jnp.bfloat16),
            pltpu.VMEM((half, block), jnp.bfloat16),
            pltpu.VMEM((half, block), jnp.bfloat16),
            pltpu.VMEM((length, block), jnp.bfloat16),
            DMA((3,)), DMA((2, PIECES)), DMA, DMA, DMA,
        ],
        compiler_params=pltpu.CompilerParams(
            collective_id=0, has_side_effects=True, vmem_limit_bytes=20 << 20
        ),
        cost_estimate=BUSY,
        name="solve",
    )(rhs, inverse, own, got, after)


def gather_kernel(
    own_piece, taken, full, rest,
    mine, cross, x_send, x_recv, send_sem, recv_sem, core_send, core_recv,
):
    row, _, core, x_hi, z, y = place()
    half = cross.shape[0]
    has_cross = core == row
    steps = range(1, SIDE)

    for h, (kept, crossed) in enumerate(((own_piece, taken), (taken, own_piece))):
        @pl.when(x_hi == h)
        def _():
            here = piece_rows(h, z, y, half)
            mine[core, here, :] = kept[...]

            @pl.when(has_cross)
            def _():
                cross[here, :] = crossed[...]

    side = at(z, y, 1 - x_hi, core)
    greet(1 - row, side)
    greet(row, at(z, y, x_hi, 1 - core))
    for d in steps:
        greet(row, at(z, lax.rem(y + d, SIDE), x_hi, core))
        greet(row, at(lax.rem(z + d, SIDE), y, x_hi, core))
    pl.semaphore_wait(pltpu.get_barrier_semaphore(), 8)

    def x_copy(which, h, source):
        to = piece_rows(h, z, y, half)
        return remote(
            source, cross.at[to] if which else mine.at[core, to],
            x_send.at[which], x_recv.at[which], 1 - row, side,
        )

    for h, (kept, crossed) in enumerate(((own_piece, taken), (taken, own_piece))):
        @pl.when(x_hi == h)
        def _():
            x_copy(0, h, crossed).start()

            @pl.when(~has_cross)
            def _():
                x_copy(1, h, kept).start()

    for h in range(2):
        @pl.when(x_hi == 1 - h)
        def _():
            x_copy(0, h, taken).wait_recv()

            @pl.when(has_cross)
            def _():
                x_copy(1, h, taken).wait_recv()

    def copy(which, h, stage, d, back=False):
        buffer = cross if which else mine.at[core]
        along_y = (h == 0) == (stage == 0)
        turn = SIDE - d if back else d
        y_, z_ = (lax.rem(y + turn, SIDE), z) if along_y else (y, lax.rem(z + turn, SIDE))
        from_y, from_z = (y_, z_) if back else (y, z)
        if stage == 0:
            part = piece_rows(h, from_z, from_y, half)
        else:
            group = from_z if h == 0 else from_y
            part = pl.ds(
                pl.multiple_of(h * (half // 2) + group * (half // 8), half // 8), half // 8
            )
        y_to, z_to = (lax.rem(y + d, SIDE), z) if along_y else (y, lax.rem(z + d, SIDE))
        return remote(
            buffer.at[part], buffer.at[part],
            send_sem.at[which, h, stage, d - 1], recv_sem.at[which, h, stage, d - 1],
            row, at(z_to, y_to, x_hi, core),
        )

    def start(which, stage, h):
        for d in steps:
            copy(which, h, stage, d).start()

    def arrive(which, stage, h):
        for d in steps:
            copy(which, h, stage, d, True).wait_recv()

    for h in range(2):
        start(0, 0, h)

    @pl.when(has_cross)
    def _():
        for h in range(2):
            start(1, 0, h)

    for h in range(2):
        arrive(0, 0, h)
        start(0, 1, h)

    @pl.when(has_cross)
    def _():
        for h in range(2):
            arrive(1, 0, h)
            start(1, 1, h)

    buddy = at(z, y, x_hi, 1 - core)

    def share(which, h, take=False):
        part = pl.ds(h * (half // 2), half // 2)
        buffer = cross if which else mine.at[1 - core if take else core]
        return remote(
            buffer.at[part], buffer.at[part], core_send.at[which, h], core_recv.at[which, h],
            row, buddy,
        )

    for h in range(2):
        arrive(0, 1, h)
        share(0, h).start()

    @pl.when(has_cross)
    def _():
        for h in range(2):
            arrive(1, 1, h)
            share(1, h).start()

    for h in range(2):
        share(0, h, True).wait_recv()

    @pl.when(~has_cross)
    def _():
        for h in range(2):
            share(1, h, True).wait_recv()

    full[rows(row, half), :] = mine[row]
    full[rows(1 - row, half), :] = cross[...]
    rest[...] = mine[1 - row]

    def sent(which):
        for h in range(2):
            share(which, h).wait_send()
            for stage in range(2):
                for d in steps:
                    copy(which, h, stage, d).wait_send()

    sent(0)

    @pl.when(has_cross)
    def _():
        sent(1)

    x_copy(0, 0, taken).wait_send()

    @pl.when(~has_cross)
    def _():
        x_copy(1, 0, taken).wait_send()


def gather_pieces(piece, taken):
    length, block = piece.shape
    half = length * 2 * PIECES
    return pl.pallas_call(
        gather_kernel,
        out_shape=(
            pltpu.VMEM((2 * half, block), jnp.bfloat16),
            pltpu.VMEM((half, block), jnp.bfloat16),
        ),
        in_specs=[VMEM] * 2,
        out_specs=(VMEM, VMEM),
        scratch_shapes=[
            pltpu.VMEM((2, half, block), jnp.bfloat16),
            pltpu.VMEM((half, block), jnp.bfloat16),
            DMA((2,)), DMA((2,)), DMA((2, 2, 2, 3)), DMA((2, 2, 2, 3)), DMA((2, 2)), DMA((2, 2)),
        ],
        compiler_params=pltpu.CompilerParams(
            collective_id=2, has_side_effects=True, vmem_limit_bytes=12 << 20
        ),
        cost_estimate=BUSY,
        name="gather",
    )(piece, taken)


def chunk_of(length):
    return 256 if length % 256 == 0 else 128


def begin_kernel(held, full, rest, *refs, count, early):
    owns, parts, got = refs[:count], refs[count : count + early], refs[count + early]
    updated, solved, ahead, work, store_sem = refs[count + early + 1 :]
    row, col = lax.axis_index("row"), lax.axis_index("col")
    block = rest.shape[0]
    ready = work.shape[1]

    put_solved = pltpu.make_async_copy(full, solved, store_sem.at[0])
    put_solved.start()

    def store(index, start, length):
        part = pl.ds(start, length)
        return pltpu.make_async_copy(
            work.at[:, part], updated.at[:, part], store_sem.at[1 + index]
        )

    def step(i, start, mine, theirs):
        chunk = chunk_of(mine.shape[0])
        here = rows(i, chunk)
        column = pl.ds(pl.multiple_of(start + i * chunk, chunk), chunk)
        own = mine[here, :]
        if start == 0:
            own = jnp.where((col < 2) & (row >= col), jnp.zeros_like(own), own)
        total = lax.dot_general(
            full[rows(row, block), :], own, NT, preferred_element_type=jnp.float32
        )
        if theirs is None:
            ahead[:, pl.ds(pl.multiple_of(start + i * chunk - ready, chunk), chunk)] = (
                held[:, column] - total
            )
            return
        other = theirs[here, :]
        if start == 0:
            other = jnp.where(lax.rem(col, 2) == 1, got[here, :], other)
            other = jnp.where((col < 2) & (1 - row >= col), jnp.zeros_like(other), other)
        total += lax.dot_general(rest[...], other, NT, preferred_element_type=jnp.float32)
        work[:, column] = held[:, column] - total

    start = 0
    stores = []
    for index, mine in enumerate(owns):
        length = mine.shape[0]
        theirs = parts[index] if index < early else None
        pl.loop(0, length // chunk_of(length))(
            functools.partial(step, start=start, mine=mine, theirs=theirs)
        )
        if index < early:
            stores.append(store(index, start, length))
            stores[-1].start()
        start += length

    put_solved.wait()
    for copy in stores:
        copy.wait()


def begin(held, full, rest, owns, parts, got):
    half, rows_dev = held.shape
    ready = sum(part.shape[0] for part in parts)
    return pl.pallas_call(
        functools.partial(begin_kernel, count=len(owns), early=len(parts)),
        out_shape=(
            pltpu.HBM(held.shape, jnp.float32),
            pltpu.HBM(full.shape, full.dtype),
            pltpu.VMEM((half, rows_dev - ready), jnp.float32),
        ),
        in_specs=[VMEM] * (4 + len(owns) + len(parts)),
        out_specs=(HBM, HBM, VMEM),
        scratch_shapes=[
            pltpu.VMEM((half, ready), jnp.float32),
            DMA((1 + len(parts),)),
        ],
        compiler_params=pltpu.CompilerParams(vmem_limit_bytes=32 << 20),
        cost_estimate=BUSY,
        name="begin",
    )(held, full, rest, *owns, *parts, got)


def finish_kernel(start, offset, held, ahead, part, rest, updated, work, store_sem):
    length = part.shape[0]
    chunk = chunk_of(length)
    stores = []
    for j in range(length // chunk):
        here = pl.ds(j * chunk, chunk)
        total = lax.dot_general(
            rest[...], part[here, :], NT, preferred_element_type=jnp.float32
        )
        work[:, here] = ahead[:, pl.ds(offset + j * chunk, chunk)] - total
        stores.append(
            pltpu.make_async_copy(
                work.at[:, here], updated.at[:, pl.ds(start + j * chunk, chunk)], store_sem.at[j]
            )
        )
        stores[-1].start()
    for copy in stores:
        copy.wait()


def finish(updated, ahead, part, rest, start, offset):
    length = part.shape[0]
    return pl.pallas_call(
        functools.partial(finish_kernel, start, offset),
        out_shape=pltpu.HBM(updated.shape, updated.dtype),
        in_specs=[HBM, VMEM, VMEM, VMEM],
        out_specs=HBM,
        scratch_shapes=[
            pltpu.VMEM((ahead.shape[0], length), jnp.float32),
            DMA((length // chunk_of(length),)),
        ],
        input_output_aliases={0: 0},
        compiler_params=pltpu.CompilerParams(vmem_limit_bytes=12 << 20),
        cost_estimate=pl.CostEstimate(flops=10**9, bytes_accessed=10**6, transcendentals=0),
    )(updated, ahead, part, rest)


def swap(value, takes):
    col_count = lax.axis_size("col")
    pairs = [
        (row * col_count + col, (1 - row) * col_count + col)
        for row in range(2) for col in range(col_count) if takes(col)
    ]
    taken = lax.ppermute(value, ("row", "col"), pairs)
    return pltpu.with_memory_space_constraint(taken, pltpu.VMEM)


def shards(panel, rhs, inverse):
    panel, rhs, inverse = (
        pltpu.with_memory_space_constraint(value, pltpu.HBM) for value in (panel, rhs, inverse)
    )
    count = len(PARTS)
    starts = [sum(PARTS[:i]) for i in range(count)]
    sent, got = lead(panel, PARTS)
    arrived = [swap(sent[i], lambda col: i > 0 or (col % 2 == 0 and col > 0)) for i in range(count)]
    held, piece = solve_pieces(rhs, inverse, sent[0], got, sent[1])
    taken = swap(piece, lambda col: True)
    full, rest = gather_pieces(piece, taken)
    updated, solved, ahead = begin(held, full, rest, sent, arrived[:EARLY], got)
    for i in range(EARLY, count):
        updated = finish(updated, ahead, arrived[i], rest, starts[i], starts[i] - starts[EARLY])
    return solved, updated


def solution(mesh):
    return jax.shard_map(
        shards,
        mesh=mesh,
        in_specs=(P("col", "row"), P("row", "col"), P()),
        out_specs=(P(None, "row"), P("row", "col")),
        check_vma=False,
    )
```

```python
import functools

import jax
import jax.numpy as jnp
from jax import lax
from jax.experimental import pallas as pl
from jax.experimental.pallas import tpu as pltpu
from jax.sharding import PartitionSpec as P


MESH = pl.DeviceIdType.MESH
NT = (((1,), (1,)), ((), ()))
SIDE = 4
PIECES = SIDE * SIDE
PARTS = (256, 256, 768, 768, 640, 256, 128)
LEAD = 2
EARLY = 3
DMA = pltpu.SemaphoreType.DMA
HBM = pl.BlockSpec(memory_space=pltpu.HBM)
VMEM = pl.BlockSpec(memory_space=pltpu.VMEM)
ANY = pl.BlockSpec(memory_space=pl.ANY)
BUSY = pl.CostEstimate(flops=10**10, bytes_accessed=10**6, transcendentals=0)


def place():
    row = lax.axis_index("row")
    col = lax.axis_index("col")
    piece = col // 4
    return row, col, lax.rem(col, 2), lax.rem(col // 2, 2), piece // SIDE, lax.rem(piece, SIDE)


def at(z, y, x, core):
    return ((z * SIDE + y) * 2 + x) * 2 + core


def remote(src, dst, send, recv, row, col):
    return pltpu.make_async_remote_copy(
        src_ref=src, dst_ref=dst, send_sem=send, recv_sem=recv,
        device_id=(row, col), device_id_type=MESH,
    )


def greet(row, col):
    pl.semaphore_signal(
        pltpu.get_barrier_semaphore(), inc=1, device_id=(row, col), device_id_type=MESH
    )


def rows(i, length):
    return pl.ds(pl.multiple_of(i * length, length), length)


def lead_kernel(panel, *refs):
    load_sem, send_sem, recv_sem = refs[-3:]
    parts, got = refs[: -3 - LEAD], refs[-3 - LEAD : -3]
    row, col, core, _, _, _ = place()
    loads = []
    start = 0
    for i, part in enumerate(parts):
        loads.append(
            pltpu.make_async_copy(panel.at[pl.ds(start, part.shape[0])], part, load_sem.at[i])
        )
        start += part.shape[0]
    copies = [
        remote(parts[i], got[i], send_sem.at[i], recv_sem.at[i], 1 - row, col)
        for i in range(LEAD)
    ]
    for load in loads[:LEAD]:
        load.start()

    @pl.when(col > 0)
    def _():
        greet(1 - row, col)
        pl.semaphore_wait(pltpu.get_barrier_semaphore(), 1)

    loads[0].wait()

    @pl.when(col > 0)
    def _():
        copies[0].start()

    loads[1].wait()

    @pl.when(core == 1)
    def _():
        copies[1].start()

    for load in loads[LEAD:]:
        load.start()
    for load in loads[LEAD:]:
        load.wait()

    @pl.when(col > 0)
    def _():
        copies[0].wait()

    @pl.when(core == 1)
    def _():
        copies[1].wait()


def lead(panel, lengths):
    parts = tuple(pltpu.VMEM((length, panel.shape[1]), panel.dtype) for length in lengths)
    outs = pl.pallas_call(
        lead_kernel,
        out_shape=parts + parts[:LEAD],
        in_specs=[HBM],
        out_specs=(VMEM,) * (len(parts) + LEAD),
        scratch_shapes=[DMA((len(lengths),)), DMA((LEAD,)), DMA((LEAD,))],
        compiler_params=pltpu.CompilerParams(
            collective_id=1, has_side_effects=True, vmem_limit_bytes=8 << 20
        ),
        name="lead",
    )(panel)
    return outs[: len(parts)], outs[len(parts) :]


def solve(value, before, below, inv, made):
    rest = value[:, : made.shape[1]]
    if below is not None:
        rest = rest - lax.dot_general(
            before[...], jnp.concatenate([part[...] for part in below], axis=0), NT, preferred_element_type=jnp.float32
        )
    high = rest.astype(jnp.bfloat16)
    rest = rest - high.astype(jnp.float32)
    middle = rest.astype(jnp.bfloat16)
    low = (rest - middle.astype(jnp.float32)).astype(jnp.bfloat16)
    total = lax.dot_general(low, inv[...], NT, preferred_element_type=jnp.float32)
    total += lax.dot_general(middle, inv[...], NT, preferred_element_type=jnp.float32)
    total += lax.dot_general(high, inv[...], NT, preferred_element_type=jnp.float32)
    made[...] = total.astype(jnp.bfloat16)


def piece_rows(h, z, y, half):
    length = half // (2 * PIECES)
    index = z * SIDE + y if h == 0 else y * SIDE + z
    return pl.ds(pl.multiple_of(h * (half // 2) + index * length, length), length)


def scatter_copy(h, p, made, land, send, recv, row, core):
    source = made.at[piece_rows(h, p // SIDE, lax.rem(p, SIDE), made.shape[0])]
    to_row = row if h == 0 else 1 - row
    return remote(source, land, send.at[h, p], recv, to_row, p * 4 + 2 * h + core)


def solve_kernel(
    rhs, inverse, *refs,
):
    own, got = refs[:LEAD], refs[LEAD : 2 * LEAD]
    solve_body(rhs, inverse, own, got, *refs[2 * LEAD + 1 :])


def solve_body(
    rhs, inverse, own, got, held, piece_out,
    inv, made, before, land, load_sem, scatter_send, scatter_recv, before_send, before_recv,
):
    row, col, core, x_hi, _, _ = place()
    piece = col // 4
    block = inv.shape[0]
    load_value = pltpu.make_async_copy(
        rhs.at[:, pl.ds(0, block)], held.at[:, pl.ds(0, block)], load_sem.at[0]
    )
    others = pl.ds(block, rhs.shape[1] - block)
    load_others = pltpu.make_async_copy(rhs.at[:, others], held.at[:, others], load_sem.at[1])
    load_value.start()
    before_copy = remote(made, before, before_send, before_recv, row, 1)

    @pl.when(col < 2)
    def _():
        load_inv = pltpu.make_async_copy(inverse.at[core], inv, load_sem.at[2])
        load_inv.start()
        load_others.start()
        greet(row, 1 - core)

        @pl.loop(1, PIECES)
        def _(p):
            greet(row, p * 4 + core)

        @pl.loop(0, PIECES)
        def _(p):
            greet(1 - row, p * 4 + 2 + core)

        load_value.wait()
        load_inv.wait()

        @pl.when(col == 0)
        def _():
            solve(held, None, None, inv, made)

        pl.semaphore_wait(pltpu.get_barrier_semaphore(), 2 * PIECES)

        @pl.when(col == 0)
        def _():
            before_copy.start()

        @pl.when(col == 1)
        def _():
            before_copy.wait_recv()

            @pl.when(row == 0)
            def _():
                solve(held, before, own, inv, made)

            @pl.when(row == 1)
            def _():
                solve(held, before, got, inv, made)

        def scattered(act):
            @pl.loop(1, PIECES)
            def _(p):
                act(scatter_copy(0, p, made, land, scatter_send, scatter_recv, row, core))

            @pl.loop(0, PIECES)
            def _(p):
                act(scatter_copy(1, p, made, land, scatter_send, scatter_recv, row, core))

        scattered(lambda copy: copy.start())
        piece_out[...] = made[piece_rows(0, 0, 0, made.shape[0]), :]

        @pl.when(col == 0)
        def _():
            before_copy.wait_send()

        scattered(lambda copy: copy.wait_send())

    @pl.when(col >= 2)
    def _():
        load_others.start()
        load_value.wait()
        source_row = jnp.where(x_hi == 0, row, 1 - row)
        greet(source_row, core)
        pl.semaphore_wait(pltpu.get_barrier_semaphore(), 1)
        scatter_copy(0, piece, made, land, scatter_send, scatter_recv, row, core).wait_recv()
        piece_out[...] = land[...]

    load_others.wait()


def solve_pieces(rhs, inverse, own, got, after):
    half, block = rhs.shape[0], inverse.shape[1]
    length = half // (2 * PIECES)
    return pl.pallas_call(
        solve_kernel,
        out_shape=(
            pltpu.VMEM(rhs.shape, rhs.dtype),
            pltpu.VMEM((length, block), jnp.bfloat16),
        ),
        in_specs=[HBM] * 2 + [VMEM] * (2 * LEAD) + [ANY],
        out_specs=(VMEM, VMEM),
        scratch_shapes=[
            pltpu.VMEM((block, block), jnp.bfloat16),
            pltpu.VMEM((half, block), jnp.bfloat16),
            pltpu.VMEM((half, block), jnp.bfloat16),
            pltpu.VMEM((length, block), jnp.bfloat16),
            DMA((3,)), DMA((2, PIECES)), DMA, DMA, DMA,
        ],
        compiler_params=pltpu.CompilerParams(
            collective_id=0, has_side_effects=True, vmem_limit_bytes=20 << 20
        ),
        cost_estimate=BUSY,
        name="solve",
    )(rhs, inverse, *own, *got, after)


def gather_kernel(
    own_piece, taken, full, rest,
    mine, cross, x_send, x_recv, send_sem, recv_sem, core_send, core_recv,
):
    row, _, core, x_hi, z, y = place()
    half = cross.shape[0]
    has_cross = core == row
    steps = range(1, SIDE)

    for h, (kept, crossed) in enumerate(((own_piece, taken), (taken, own_piece))):
        @pl.when(x_hi == h)
        def _():
            here = piece_rows(h, z, y, half)
            mine[core, here, :] = kept[...]

            @pl.when(has_cross)
            def _():
                cross[here, :] = crossed[...]

    side = at(z, y, 1 - x_hi, core)
    greet(1 - row, side)
    greet(row, at(z, y, x_hi, 1 - core))
    for d in steps:
        greet(row, at(z, lax.rem(y + d, SIDE), x_hi, core))
        greet(row, at(lax.rem(z + d, SIDE), y, x_hi, core))
    pl.semaphore_wait(pltpu.get_barrier_semaphore(), 8)

    def x_copy(which, h, source):
        to = piece_rows(h, z, y, half)
        return remote(
            source, cross.at[to] if which else mine.at[core, to],
            x_send.at[which], x_recv.at[which], 1 - row, side,
        )

    for h, (kept, crossed) in enumerate(((own_piece, taken), (taken, own_piece))):
        @pl.when(x_hi == h)
        def _():
            x_copy(0, h, crossed).start()

            @pl.when(~has_cross)
            def _():
                x_copy(1, h, kept).start()

    for h in range(2):
        @pl.when(x_hi == 1 - h)
        def _():
            x_copy(0, h, taken).wait_recv()

            @pl.when(has_cross)
            def _():
                x_copy(1, h, taken).wait_recv()

    def copy(which, h, stage, d, back=False):
        buffer = cross if which else mine.at[core]
        along_y = (h == 0) == (stage == 0)
        turn = SIDE - d if back else d
        y_, z_ = (lax.rem(y + turn, SIDE), z) if along_y else (y, lax.rem(z + turn, SIDE))
        from_y, from_z = (y_, z_) if back else (y, z)
        if stage == 0:
            part = piece_rows(h, from_z, from_y, half)
        else:
            group = from_z if h == 0 else from_y
            part = pl.ds(
                pl.multiple_of(h * (half // 2) + group * (half // 8), half // 8), half // 8
            )
        y_to, z_to = (lax.rem(y + d, SIDE), z) if along_y else (y, lax.rem(z + d, SIDE))
        return remote(
            buffer.at[part], buffer.at[part],
            send_sem.at[which, h, stage, d - 1], recv_sem.at[which, h, stage, d - 1],
            row, at(z_to, y_to, x_hi, core),
        )

    def start(which, stage, h):
        for d in steps:
            copy(which, h, stage, d).start()

    def arrive(which, stage, h):
        for d in steps:
            copy(which, h, stage, d, True).wait_recv()

    for h in range(2):
        start(0, 0, h)

    @pl.when(has_cross)
    def _():
        for h in range(2):
            start(1, 0, h)

    for h in range(2):
        arrive(0, 0, h)
        start(0, 1, h)

    @pl.when(has_cross)
    def _():
        for h in range(2):
            arrive(1, 0, h)
            start(1, 1, h)

    buddy = at(z, y, x_hi, 1 - core)

    def share(which, h, take=False):
        part = pl.ds(h * (half // 2), half // 2)
        buffer = cross if which else mine.at[1 - core if take else core]
        return remote(
            buffer.at[part], buffer.at[part], core_send.at[which, h], core_recv.at[which, h],
            row, buddy,
        )

    for h in range(2):
        arrive(0, 1, h)
        share(0, h).start()

    @pl.when(has_cross)
    def _():
        for h in range(2):
            arrive(1, 1, h)
            share(1, h).start()

    for h in range(2):
        share(0, h, True).wait_recv()

    @pl.when(~has_cross)
    def _():
        for h in range(2):
            share(1, h, True).wait_recv()

    full[rows(row, half), :] = mine[row]
    full[rows(1 - row, half), :] = cross[...]
    rest[...] = mine[1 - row]

    def sent(which):
        for h in range(2):
            share(which, h).wait_send()
            for stage in range(2):
                for d in steps:
                    copy(which, h, stage, d).wait_send()

    sent(0)

    @pl.when(has_cross)
    def _():
        sent(1)

    x_copy(0, 0, taken).wait_send()

    @pl.when(~has_cross)
    def _():
        x_copy(1, 0, taken).wait_send()


def gather_pieces(piece, taken):
    length, block = piece.shape
    half = length * 2 * PIECES
    return pl.pallas_call(
        gather_kernel,
        out_shape=(
            pltpu.VMEM((2 * half, block), jnp.bfloat16),
            pltpu.VMEM((half, block), jnp.bfloat16),
        ),
        in_specs=[VMEM] * 2,
        out_specs=(VMEM, VMEM),
        scratch_shapes=[
            pltpu.VMEM((2, half, block), jnp.bfloat16),
            pltpu.VMEM((half, block), jnp.bfloat16),
            DMA((2,)), DMA((2,)), DMA((2, 2, 2, 3)), DMA((2, 2, 2, 3)), DMA((2, 2)), DMA((2, 2)),
        ],
        compiler_params=pltpu.CompilerParams(
            collective_id=2, has_side_effects=True, vmem_limit_bytes=12 << 20
        ),
        cost_estimate=BUSY,
        name="gather",
    )(piece, taken)


def chunk_of(length):
    return 256 if length % 256 == 0 else 128


def begin_kernel(held, full, rest, *refs, count, early):
    owns, parts = refs[:count], refs[count : count + early]
    got = refs[count + early : count + early + LEAD]
    updated, solved, ahead, work, store_sem = refs[count + early + LEAD :]
    row, col = lax.axis_index("row"), lax.axis_index("col")
    block = rest.shape[0]
    ready = work.shape[1]

    put_solved = pltpu.make_async_copy(full, solved, store_sem.at[0])
    put_solved.start()

    def store(index, start, length):
        part = pl.ds(start, length)
        return pltpu.make_async_copy(
            work.at[:, part], updated.at[:, part], store_sem.at[1 + index]
        )

    def step(i, start, mine, theirs, led):
        chunk = chunk_of(mine.shape[0])
        here = rows(i, chunk)
        column = pl.ds(pl.multiple_of(start + i * chunk, chunk), chunk)
        own = mine[here, :]
        if start < block:
            own = jnp.where((col < 2) & (row >= col), jnp.zeros_like(own), own)
        total = lax.dot_general(
            full[rows(row, block), :], own, NT, preferred_element_type=jnp.float32
        )
        if theirs is None:
            ahead[:, pl.ds(pl.multiple_of(start + i * chunk - ready, chunk), chunk)] = (
                held[:, column] - total
            )
            return
        other = theirs[here, :]
        if led is not None:
            other = jnp.where(lax.rem(col, 2) == 1, led[here, :], other)
        if start < block:
            other = jnp.where((col < 2) & (1 - row >= col), jnp.zeros_like(other), other)
        total += lax.dot_general(rest[...], other, NT, preferred_element_type=jnp.float32)
        work[:, column] = held[:, column] - total

    start = 0
    stores = []
    for index, mine in enumerate(owns):
        length = mine.shape[0]
        theirs = parts[index - 1] if 0 < index <= early else None
        led = got[index] if 0 < index < LEAD else None
        if index == 0:
            theirs = got[0]
        pl.loop(0, length // chunk_of(length))(
            functools.partial(step, start=start, mine=mine, theirs=theirs, led=led)
        )
        if index <= early:
            stores.append(store(index, start, length))
            stores[-1].start()
        start += length

    put_solved.wait()
    for copy in stores:
        copy.wait()


def begin(held, full, rest, owns, parts, got):
    half, rows_dev = held.shape
    ready = got[0].shape[0] + sum(part.shape[0] for part in parts)
    return pl.pallas_call(
        functools.partial(begin_kernel, count=len(owns), early=len(parts)),
        out_shape=(
            pltpu.HBM(held.shape, jnp.float32),
            pltpu.HBM(full.shape, full.dtype),
            pltpu.VMEM((half, rows_dev - ready), jnp.float32),
        ),
        in_specs=[VMEM] * (3 + LEAD + len(owns) + len(parts)),
        out_specs=(HBM, HBM, VMEM),
        scratch_shapes=[
            pltpu.VMEM((half, ready), jnp.float32),
            DMA((2 + len(parts),)),
        ],
        compiler_params=pltpu.CompilerParams(vmem_limit_bytes=32 << 20),
        cost_estimate=BUSY,
        name="begin",
    )(held, full, rest, *owns, *parts, *got)


def finish_kernel(start, offset, held, ahead, part, rest, updated, work, store_sem):
    length = part.shape[0]
    chunk = chunk_of(length)
    half = work.shape[0] // 2
    stores = []
    for j in range(length // chunk):
        here = pl.ds(j * chunk, chunk)
        there = pl.ds(start + j * chunk, chunk)
        for h in range(2):
            tall = pl.ds(h * half, half)
            total = lax.dot_general(
                rest[tall, :], part[here, :], NT, preferred_element_type=jnp.float32
            )
            work[tall, here] = ahead[tall, pl.ds(offset + j * chunk, chunk)] - total
            stores.append(
                pltpu.make_async_copy(
                    work.at[tall, here], updated.at[tall, there], store_sem.at[2 * j + h]
                )
            )
            stores[-1].start()
    for copy in stores:
        copy.wait()


def finish(updated, ahead, part, rest, start, offset):
    length = part.shape[0]
    return pl.pallas_call(
        functools.partial(finish_kernel, start, offset),
        out_shape=pltpu.HBM(updated.shape, updated.dtype),
        in_specs=[HBM, VMEM, VMEM, VMEM],
        out_specs=HBM,
        scratch_shapes=[
            pltpu.VMEM((ahead.shape[0], length), jnp.float32),
            DMA((2 * length // chunk_of(length),)),
        ],
        input_output_aliases={0: 0},
        compiler_params=pltpu.CompilerParams(vmem_limit_bytes=12 << 20),
        cost_estimate=pl.CostEstimate(flops=10**9, bytes_accessed=10**6, transcendentals=0),
    )(updated, ahead, part, rest)


def swap(value, takes):
    col_count = lax.axis_size("col")
    pairs = [
        (row * col_count + col, (1 - row) * col_count + col)
        for row in range(2) for col in range(col_count) if takes(col)
    ]
    taken = lax.ppermute(value, ("row", "col"), pairs)
    return pltpu.with_memory_space_constraint(taken, pltpu.VMEM)


def shards(panel, rhs, inverse):
    panel, rhs, inverse = (
        pltpu.with_memory_space_constraint(value, pltpu.HBM) for value in (panel, rhs, inverse)
    )
    count = len(PARTS)
    starts = [sum(PARTS[:i]) for i in range(count)]
    sent, got = lead(panel, PARTS)
    arrived = [got[0]]
    for i in range(1, count):
        arrived.append(swap(sent[i], lambda col: i >= LEAD or (col % 2 == 0 and col > 0)))
    held, piece = solve_pieces(rhs, inverse, sent[:LEAD], got, sent[LEAD])
    taken = swap(piece, lambda col: True)
    full, rest = gather_pieces(piece, taken)
    updated, solved, ahead = begin(held, full, rest, sent, arrived[1:EARLY], got)
    for i in range(EARLY, count):
        updated = finish(updated, ahead, arrived[i], rest, starts[i], starts[i] - starts[EARLY])
    return solved, updated


def solution(mesh):
    return jax.shard_map(
        shards,
        mesh=mesh,
        in_specs=(P("col", "row"), P("row", "col"), P()),
        out_specs=(P(None, "row"), P("row", "col")),
        check_vma=False,
    )
```

```python
import functools

import jax
import jax.numpy as jnp
from jax import lax
from jax.experimental import pallas as pl
from jax.experimental.pallas import tpu as pltpu
from jax.sharding import PartitionSpec as P


MESH = pl.DeviceIdType.MESH
NT = (((1,), (1,)), ((), ()))
SIDE = 4
PIECES = SIDE * SIDE
PARTS = (512, 768, 768, 640, 256, 128)
QUICK = 64
EARLY = 2
DMA = pltpu.SemaphoreType.DMA
HBM = pl.BlockSpec(memory_space=pltpu.HBM)
VMEM = pl.BlockSpec(memory_space=pltpu.VMEM)
ANY = pl.BlockSpec(memory_space=pl.ANY)
BUSY = pl.CostEstimate(flops=10**10, bytes_accessed=10**6, transcendentals=0)


def place():
    row = lax.axis_index("row")
    col = lax.axis_index("col")
    piece = col // 4
    return row, col, lax.rem(col, 2), lax.rem(col // 2, 2), piece // SIDE, lax.rem(piece, SIDE)


def at(z, y, x, core):
    return ((z * SIDE + y) * 2 + x) * 2 + core


def remote(src, dst, send, recv, row, col):
    return pltpu.make_async_remote_copy(
        src_ref=src, dst_ref=dst, send_sem=send, recv_sem=recv,
        device_id=(row, col), device_id_type=MESH,
    )


def greet(row, col):
    pl.semaphore_signal(
        pltpu.get_barrier_semaphore(), inc=1, device_id=(row, col), device_id_type=MESH
    )


def rows(i, length):
    return pl.ds(pl.multiple_of(i * length, length), length)


def lead_kernel(panel, *refs):
    *parts, got, load_sem, send_sem, recv_sem = refs
    row, col, core, _, _, _ = place()
    loads = []
    start = 0
    for i, part in enumerate(parts):
        loads.append(
            pltpu.make_async_copy(panel.at[pl.ds(start, part.shape[0])], part, load_sem.at[i])
        )
        start += part.shape[0]
    spans = (pl.ds(0, QUICK), pl.ds(QUICK, parts[0].shape[0] - QUICK))
    lead_loads = [
        pltpu.make_async_copy(panel.at[span], parts[0].at[span], load_sem.at[len(parts) + i])
        for i, span in enumerate(spans)
    ]
    for load in lead_loads:
        load.start()

    @pl.when(core == 1)
    def _():
        copies = [
            remote(
                parts[0].at[span], got.at[span], send_sem.at[i], recv_sem.at[i], 1 - row, col
            )
            for i, span in enumerate(spans)
        ]
        greet(1 - row, col)
        lead_loads[0].wait()
        pl.semaphore_wait(pltpu.get_barrier_semaphore(), 1)
        copies[0].start()
        lead_loads[1].wait()
        copies[1].start()
        for load in loads[1:]:
            load.start()
        for copy in copies:
            copy.wait()

    @pl.when(core == 0)
    def _():
        for load in loads[1:]:
            load.start()
        for load in lead_loads:
            load.wait()

    for load in loads[1:]:
        load.wait()


def lead(panel, lengths):
    parts = [pltpu.VMEM((length, panel.shape[1]), panel.dtype) for length in lengths]
    *parts, got = pl.pallas_call(
        lead_kernel,
        out_shape=(*parts, parts[0]),
        in_specs=[HBM],
        out_specs=(VMEM,) * (len(parts) + 1),
        scratch_shapes=[DMA((len(lengths) + 2,)), DMA((2,)), DMA((2,))],
        compiler_params=pltpu.CompilerParams(
            collective_id=1, has_side_effects=True, vmem_limit_bytes=8 << 20
        ),
        name="lead",
    )(panel)
    return parts, got


def solve(value, before, below, inv, made):
    rest = value[:, : made.shape[1]]
    if below is not None:
        rest = rest - lax.dot_general(
            before[...], below[...], NT, preferred_element_type=jnp.float32
        )
    high = rest.astype(jnp.bfloat16)
    rest = rest - high.astype(jnp.float32)
    middle = rest.astype(jnp.bfloat16)
    low = (rest - middle.astype(jnp.float32)).astype(jnp.bfloat16)
    total = lax.dot_general(low, inv[...], NT, preferred_element_type=jnp.float32)
    total += lax.dot_general(middle, inv[...], NT, preferred_element_type=jnp.float32)
    total += lax.dot_general(high, inv[...], NT, preferred_element_type=jnp.float32)
    made[...] = total.astype(jnp.bfloat16)


def piece_rows(h, z, y, half):
    length = half // (2 * PIECES)
    index = z * SIDE + y if h == 0 else y * SIDE + z
    return pl.ds(pl.multiple_of(h * (half // 2) + index * length, length), length)


def scatter_copy(h, p, made, land, send, recv, row, core):
    source = made.at[piece_rows(h, p // SIDE, lax.rem(p, SIDE), made.shape[0])]
    to_row = row if h == 0 else 1 - row
    return remote(source, land, send.at[h, p], recv, to_row, p * 4 + 2 * h + core)


def solve_kernel(
    rhs, inverse, own, got, after, held, piece_out,
    inv, made, before, land, load_sem, scatter_send, scatter_recv, before_send, before_recv,
):
    row, col, core, x_hi, _, _ = place()
    piece = col // 4
    block = inv.shape[0]
    load_value = pltpu.make_async_copy(
        rhs.at[:, pl.ds(0, block)], held.at[:, pl.ds(0, block)], load_sem.at[0]
    )
    others = pl.ds(block, rhs.shape[1] - block)
    load_others = pltpu.make_async_copy(rhs.at[:, others], held.at[:, others], load_sem.at[1])
    load_value.start()
    before_copy = remote(made, before, before_send, before_recv, row, 1)

    @pl.when(col < 2)
    def _():
        load_inv = pltpu.make_async_copy(inverse.at[core], inv, load_sem.at[2])
        load_inv.start()
        load_others.start()
        greet(row, 1 - core)

        @pl.loop(1, PIECES)
        def _(p):
            greet(row, p * 4 + core)

        @pl.loop(0, PIECES)
        def _(p):
            greet(1 - row, p * 4 + 2 + core)

        load_value.wait()
        load_inv.wait()

        @pl.when(col == 0)
        def _():
            solve(held, None, None, inv, made)

        pl.semaphore_wait(pltpu.get_barrier_semaphore(), 2 * PIECES)

        @pl.when(col == 0)
        def _():
            before_copy.start()

        @pl.when(col == 1)
        def _():
            before_copy.wait_recv()

            @pl.when(row == 0)
            def _():
                solve(held, before, own, inv, made)

            @pl.when(row == 1)
            def _():
                solve(held, before, got, inv, made)

        def scattered(act):
            @pl.loop(1, PIECES)
            def _(p):
                act(scatter_copy(0, p, made, land, scatter_send, scatter_recv, row, core))

            @pl.loop(0, PIECES)
            def _(p):
                act(scatter_copy(1, p, made, land, scatter_send, scatter_recv, row, core))

        scattered(lambda copy: copy.start())
        piece_out[...] = made[piece_rows(0, 0, 0, made.shape[0]), :]

        @pl.when(col == 0)
        def _():
            before_copy.wait_send()

        scattered(lambda copy: copy.wait_send())

    @pl.when(col >= 2)
    def _():
        load_others.start()
        load_value.wait()
        source_row = jnp.where(x_hi == 0, row, 1 - row)
        greet(source_row, core)
        pl.semaphore_wait(pltpu.get_barrier_semaphore(), 1)
        scatter_copy(0, piece, made, land, scatter_send, scatter_recv, row, core).wait_recv()
        piece_out[...] = land[...]

    load_others.wait()


def solve_pieces(rhs, inverse, own, got, after):
    half, block = rhs.shape[0], inverse.shape[1]
    length = half // (2 * PIECES)
    return pl.pallas_call(
        solve_kernel,
        out_shape=(
            pltpu.VMEM(rhs.shape, rhs.dtype),
            pltpu.VMEM((length, block), jnp.bfloat16),
        ),
        in_specs=[HBM] * 2 + [VMEM] * 2 + [ANY],
        out_specs=(VMEM, VMEM),
        scratch_shapes=[
            pltpu.VMEM((block, block), jnp.bfloat16),
            pltpu.VMEM((half, block), jnp.bfloat16),
            pltpu.VMEM((half, block), jnp.bfloat16),
            pltpu.VMEM((length, block), jnp.bfloat16),
            DMA((3,)), DMA((2, PIECES)), DMA, DMA, DMA,
        ],
        compiler_params=pltpu.CompilerParams(
            collective_id=0, has_side_effects=True, vmem_limit_bytes=20 << 20
        ),
        cost_estimate=BUSY,
        name="solve",
    )(rhs, inverse, own, got, after)


def gather_kernel(
    own_piece, taken, full, rest,
    mine, cross, x_send, x_recv, send_sem, recv_sem, core_send, core_recv,
):
    row, _, core, x_hi, z, y = place()
    half = cross.shape[0]
    has_cross = core == row
    steps = range(1, SIDE)

    for h, (kept, crossed) in enumerate(((own_piece, taken), (taken, own_piece))):
        @pl.when(x_hi == h)
        def _():
            here = piece_rows(h, z, y, half)
            mine[core, here, :] = kept[...]

            @pl.when(has_cross)
            def _():
                cross[here, :] = crossed[...]

    side = at(z, y, 1 - x_hi, core)
    greet(1 - row, side)
    greet(row, at(z, y, x_hi, 1 - core))
    for d in steps:
        greet(row, at(z, lax.rem(y + d, SIDE), x_hi, core))
        greet(row, at(lax.rem(z + d, SIDE), y, x_hi, core))
    pl.semaphore_wait(pltpu.get_barrier_semaphore(), 8)

    def x_copy(which, h, source):
        to = piece_rows(h, z, y, half)
        return remote(
            source, cross.at[to] if which else mine.at[core, to],
            x_send.at[which], x_recv.at[which], 1 - row, side,
        )

    for h, (kept, crossed) in enumerate(((own_piece, taken), (taken, own_piece))):
        @pl.when(x_hi == h)
        def _():
            x_copy(0, h, crossed).start()

            @pl.when(~has_cross)
            def _():
                x_copy(1, h, kept).start()

    for h in range(2):
        @pl.when(x_hi == 1 - h)
        def _():
            x_copy(0, h, taken).wait_recv()

            @pl.when(has_cross)
            def _():
                x_copy(1, h, taken).wait_recv()

    def copy(which, h, stage, d, back=False):
        buffer = cross if which else mine.at[core]
        along_y = (h == 0) == (stage == 0)
        turn = SIDE - d if back else d
        y_, z_ = (lax.rem(y + turn, SIDE), z) if along_y else (y, lax.rem(z + turn, SIDE))
        from_y, from_z = (y_, z_) if back else (y, z)
        if stage == 0:
            part = piece_rows(h, from_z, from_y, half)
        else:
            group = from_z if h == 0 else from_y
            part = pl.ds(
                pl.multiple_of(h * (half // 2) + group * (half // 8), half // 8), half // 8
            )
        y_to, z_to = (lax.rem(y + d, SIDE), z) if along_y else (y, lax.rem(z + d, SIDE))
        return remote(
            buffer.at[part], buffer.at[part],
            send_sem.at[which, h, stage, d - 1], recv_sem.at[which, h, stage, d - 1],
            row, at(z_to, y_to, x_hi, core),
        )

    def start(which, stage, h):
        for d in steps:
            copy(which, h, stage, d).start()

    def arrive(which, stage, h):
        for d in steps:
            copy(which, h, stage, d, True).wait_recv()

    for h in range(2):
        start(0, 0, h)

    @pl.when(has_cross)
    def _():
        for h in range(2):
            start(1, 0, h)

    for h in range(2):
        arrive(0, 0, h)
        start(0, 1, h)

    @pl.when(has_cross)
    def _():
        for h in range(2):
            arrive(1, 0, h)
            start(1, 1, h)

    buddy = at(z, y, x_hi, 1 - core)

    def share(which, h, take=False):
        part = pl.ds(h * (half // 2), half // 2)
        buffer = cross if which else mine.at[1 - core if take else core]
        return remote(
            buffer.at[part], buffer.at[part], core_send.at[which, h], core_recv.at[which, h],
            row, buddy,
        )

    for h in range(2):
        arrive(0, 1, h)
        share(0, h).start()

    @pl.when(has_cross)
    def _():
        for h in range(2):
            arrive(1, 1, h)
            share(1, h).start()

    for h in range(2):
        share(0, h, True).wait_recv()

    @pl.when(~has_cross)
    def _():
        for h in range(2):
            share(1, h, True).wait_recv()

    full[rows(row, half), :] = mine[row]
    full[rows(1 - row, half), :] = cross[...]
    rest[...] = mine[1 - row]

    def sent(which):
        for h in range(2):
            share(which, h).wait_send()
            for stage in range(2):
                for d in steps:
                    copy(which, h, stage, d).wait_send()

    sent(0)

    @pl.when(has_cross)
    def _():
        sent(1)

    x_copy(0, 0, taken).wait_send()

    @pl.when(~has_cross)
    def _():
        x_copy(1, 0, taken).wait_send()


def gather_pieces(piece, taken):
    length, block = piece.shape
    half = length * 2 * PIECES
    return pl.pallas_call(
        gather_kernel,
        out_shape=(
            pltpu.VMEM((2 * half, block), jnp.bfloat16),
            pltpu.VMEM((half, block), jnp.bfloat16),
        ),
        in_specs=[VMEM] * 2,
        out_specs=(VMEM, VMEM),
        scratch_shapes=[
            pltpu.VMEM((2, half, block), jnp.bfloat16),
            pltpu.VMEM((half, block), jnp.bfloat16),
            DMA((2,)), DMA((2,)), DMA((2, 2, 2, 3)), DMA((2, 2, 2, 3)), DMA((2, 2)), DMA((2, 2)),
        ],
        compiler_params=pltpu.CompilerParams(
            collective_id=2, has_side_effects=True, vmem_limit_bytes=12 << 20
        ),
        cost_estimate=BUSY,
        name="gather",
    )(piece, taken)


def chunk_of(length):
    return 256 if length % 256 == 0 else 128


def begin_kernel(held, full, rest, *refs, count, early):
    owns, parts, got = refs[:count], refs[count : count + early], refs[count + early]
    updated, solved, ahead, work, store_sem = refs[count + early + 1 :]
    row, col = lax.axis_index("row"), lax.axis_index("col")
    block = rest.shape[0]
    ready = work.shape[1]

    put_solved = pltpu.make_async_copy(full, solved, store_sem.at[0])
    put_solved.start()

    def store(index, start, length):
        part = pl.ds(start, length)
        return pltpu.make_async_copy(
            work.at[:, part], updated.at[:, part], store_sem.at[1 + index]
        )

    def step(i, start, mine, theirs):
        chunk = chunk_of(mine.shape[0])
        here = rows(i, chunk)
        column = pl.ds(pl.multiple_of(start + i * chunk, chunk), chunk)
        own = mine[here, :]
        if start == 0:
            own = jnp.where((col < 2) & (row >= col), jnp.zeros_like(own), own)
        total = lax.dot_general(
            full[rows(row, block), :], own, NT, preferred_element_type=jnp.float32
        )
        if theirs is None:
            ahead[:, pl.ds(pl.multiple_of(start + i * chunk - ready, chunk), chunk)] = (
                held[:, column] - total
            )
            return
        other = theirs[here, :]
        if start == 0:
            other = jnp.where(lax.rem(col, 2) == 1, got[here, :], other)
            other = jnp.where((col < 2) & (1 - row >= col), jnp.zeros_like(other), other)
        total += lax.dot_general(rest[...], other, NT, preferred_element_type=jnp.float32)
        work[:, column] = held[:, column] - total

    start = 0
    stores = []
    for index, mine in enumerate(owns):
        length = mine.shape[0]
        theirs = parts[index] if index < early else None
        pl.loop(0, length // chunk_of(length))(
            functools.partial(step, start=start, mine=mine, theirs=theirs)
        )
        if index < early:
            stores.append(store(index, start, length))
            stores[-1].start()
        start += length

    put_solved.wait()
    for copy in stores:
        copy.wait()


def begin(held, full, rest, owns, parts, got):
    half, rows_dev = held.shape
    ready = sum(part.shape[0] for part in parts)
    return pl.pallas_call(
        functools.partial(begin_kernel, count=len(owns), early=len(parts)),
        out_shape=(
            pltpu.HBM(held.shape, jnp.float32),
            pltpu.HBM(full.shape, full.dtype),
            pltpu.VMEM((half, rows_dev - ready), jnp.float32),
        ),
        in_specs=[VMEM] * (4 + len(owns) + len(parts)),
        out_specs=(HBM, HBM, VMEM),
        scratch_shapes=[
            pltpu.VMEM((half, ready), jnp.float32),
            DMA((1 + len(parts),)),
        ],
        compiler_params=pltpu.CompilerParams(vmem_limit_bytes=32 << 20),
        cost_estimate=BUSY,
        name="begin",
    )(held, full, rest, *owns, *parts, got)


def finish_kernel(start, offset, held, ahead, part, rest, updated, work, store_sem):
    length = part.shape[0]
    chunk = chunk_of(length)
    stores = []
    for j in range(length // chunk):
        here = pl.ds(j * chunk, chunk)
        total = lax.dot_general(
            rest[...], part[here, :], NT, preferred_element_type=jnp.float32
        )
        work[:, here] = ahead[:, pl.ds(offset + j * chunk, chunk)] - total
        stores.append(
            pltpu.make_async_copy(
                work.at[:, here], updated.at[:, pl.ds(start + j * chunk, chunk)], store_sem.at[j]
            )
        )
        stores[-1].start()
    for copy in stores:
        copy.wait()


def finish(updated, ahead, part, rest, start, offset):
    length = part.shape[0]
    return pl.pallas_call(
        functools.partial(finish_kernel, start, offset),
        out_shape=pltpu.HBM(updated.shape, updated.dtype),
        in_specs=[HBM, VMEM, VMEM, VMEM],
        out_specs=HBM,
        scratch_shapes=[
            pltpu.VMEM((ahead.shape[0], length), jnp.float32),
            DMA((length // chunk_of(length),)),
        ],
        input_output_aliases={0: 0},
        compiler_params=pltpu.CompilerParams(vmem_limit_bytes=12 << 20),
        cost_estimate=pl.CostEstimate(flops=10**9, bytes_accessed=10**6, transcendentals=0),
    )(updated, ahead, part, rest)


def swap(value, takes):
    col_count = lax.axis_size("col")
    pairs = [
        (row * col_count + col, (1 - row) * col_count + col)
        for row in range(2) for col in range(col_count) if takes(col)
    ]
    taken = lax.ppermute(value, ("row", "col"), pairs)
    return pltpu.with_memory_space_constraint(taken, pltpu.VMEM)


def shards(panel, rhs, inverse):
    panel, rhs, inverse = (
        pltpu.with_memory_space_constraint(value, pltpu.HBM) for value in (panel, rhs, inverse)
    )
    count = len(PARTS)
    starts = [sum(PARTS[:i]) for i in range(count)]
    sent, got = lead(panel, PARTS)
    arrived = [swap(sent[i], lambda col: i > 0 or (col % 2 == 0 and col > 0)) for i in range(count)]
    held, piece = solve_pieces(rhs, inverse, sent[0], got, sent[1])
    taken = swap(piece, lambda col: True)
    full, rest = gather_pieces(piece, taken)
    updated, solved, ahead = begin(held, full, rest, sent, arrived[:EARLY], got)
    for i in range(EARLY, count):
        updated = finish(updated, ahead, arrived[i], rest, starts[i], starts[i] - starts[EARLY])
    return solved, updated


def solution(mesh):
    return jax.shard_map(
        shards,
        mesh=mesh,
        in_specs=(P("col", "row"), P("row", "col"), P()),
        out_specs=(P(None, "row"), P("row", "col")),
        check_vma=False,
    )
```

```python
import functools

import jax
import jax.numpy as jnp
from jax import lax
from jax.experimental import pallas as pl
from jax.experimental.pallas import tpu as pltpu
from jax.sharding import PartitionSpec as P


MESH = pl.DeviceIdType.MESH
NT = (((1,), (1,)), ((), ()))
SIDE = 4
PIECES = SIDE * SIDE
PARTS = (512, 768, 768, 640, 256, 128)
EARLY = 2
DMA = pltpu.SemaphoreType.DMA
HBM = pl.BlockSpec(memory_space=pltpu.HBM)
VMEM = pl.BlockSpec(memory_space=pltpu.VMEM)
ANY = pl.BlockSpec(memory_space=pl.ANY)
BUSY = pl.CostEstimate(flops=10**10, bytes_accessed=10**6, transcendentals=0)


def place():
    row = lax.axis_index("row")
    col = lax.axis_index("col")
    piece = col // 4
    return row, col, lax.rem(col, 2), lax.rem(col // 2, 2), piece // SIDE, lax.rem(piece, SIDE)


def at(z, y, x, core):
    return ((z * SIDE + y) * 2 + x) * 2 + core


def remote(src, dst, send, recv, row, col):
    return pltpu.make_async_remote_copy(
        src_ref=src, dst_ref=dst, send_sem=send, recv_sem=recv,
        device_id=(row, col), device_id_type=MESH,
    )


def greet(row, col):
    pl.semaphore_signal(
        pltpu.get_barrier_semaphore(), inc=1, device_id=(row, col), device_id_type=MESH
    )


def rows(i, length):
    return pl.ds(pl.multiple_of(i * length, length), length)


def lead_kernel(panel, *refs):
    *parts, got, load_sem, send_sem, recv_sem = refs
    row, col, core, _, _, _ = place()
    loads = []
    start = 0
    for i, part in enumerate(parts):
        loads.append(
            pltpu.make_async_copy(panel.at[pl.ds(start, part.shape[0])], part, load_sem.at[i])
        )
        start += part.shape[0]

    @pl.when(core == 1)
    def _():
        copy = remote(panel.at[pl.ds(0, got.shape[0])], got, send_sem, recv_sem, 1 - row, col)
        greet(1 - row, col)
        pl.semaphore_wait(pltpu.get_barrier_semaphore(), 1)
        copy.start()
        for load in loads:
            load.start()
        copy.wait()

    @pl.when(core == 0)
    def _():
        for load in loads:
            load.start()

    for load in loads:
        load.wait()


def lead(panel, lengths):
    parts = [pltpu.VMEM((length, panel.shape[1]), panel.dtype) for length in lengths]
    *parts, got = pl.pallas_call(
        lead_kernel,
        out_shape=(*parts, parts[0]),
        in_specs=[HBM],
        out_specs=(VMEM,) * (len(parts) + 1),
        scratch_shapes=[DMA((len(lengths),)), DMA, DMA],
        compiler_params=pltpu.CompilerParams(
            collective_id=1, has_side_effects=True, vmem_limit_bytes=8 << 20
        ),
        name="lead",
    )(panel)
    return parts, got


def solve(value, before, below, inv, made):
    rest = value[:, : made.shape[1]]
    if below is not None:
        rest = rest - lax.dot_general(
            before[...], below[...], NT, preferred_element_type=jnp.float32
        )
    high = rest.astype(jnp.bfloat16)
    rest = rest - high.astype(jnp.float32)
    middle = rest.astype(jnp.bfloat16)
    low = (rest - middle.astype(jnp.float32)).astype(jnp.bfloat16)
    total = lax.dot_general(low, inv[...], NT, preferred_element_type=jnp.float32)
    total += lax.dot_general(middle, inv[...], NT, preferred_element_type=jnp.float32)
    total += lax.dot_general(high, inv[...], NT, preferred_element_type=jnp.float32)
    made[...] = total.astype(jnp.bfloat16)


def piece_rows(h, z, y, half):
    length = half // (2 * PIECES)
    index = z * SIDE + y if h == 0 else y * SIDE + z
    return pl.ds(pl.multiple_of(h * (half // 2) + index * length, length), length)


def scatter_copy(h, p, made, land, send, recv, row, core):
    source = made.at[piece_rows(h, p // SIDE, lax.rem(p, SIDE), made.shape[0])]
    to_row = row if h == 0 else 1 - row
    return remote(source, land, send.at[h, p], recv, to_row, p * 4 + 2 * h + core)


def solve_kernel(
    rhs, inverse, own, got, after, held, piece_out,
    inv, made, before, land, load_sem, scatter_send, scatter_recv, before_send, before_recv,
):
    row, col, core, x_hi, _, _ = place()
    piece = col // 4
    block = inv.shape[0]
    load_value = pltpu.make_async_copy(
        rhs.at[:, pl.ds(0, block)], held.at[:, pl.ds(0, block)], load_sem.at[0]
    )
    others = pl.ds(block, rhs.shape[1] - block)
    load_others = pltpu.make_async_copy(rhs.at[:, others], held.at[:, others], load_sem.at[1])
    load_value.start()
    before_copy = remote(made, before, before_send, before_recv, row, 1)

    @pl.when(col < 2)
    def _():
        load_inv = pltpu.make_async_copy(inverse.at[core], inv, load_sem.at[2])
        load_inv.start()
        load_others.start()
        greet(row, 1 - core)

        @pl.loop(1, PIECES)
        def _(p):
            greet(row, p * 4 + core)

        @pl.loop(0, PIECES)
        def _(p):
            greet(1 - row, p * 4 + 2 + core)

        load_value.wait()
        load_inv.wait()

        @pl.when(col == 0)
        def _():
            solve(held, None, None, inv, made)

        pl.semaphore_wait(pltpu.get_barrier_semaphore(), 2 * PIECES)

        @pl.when(col == 0)
        def _():
            before_copy.start()

        @pl.when(col == 1)
        def _():
            before_copy.wait_recv()

            @pl.when(row == 0)
            def _():
                solve(held, before, own, inv, made)

            @pl.when(row == 1)
            def _():
                solve(held, before, got, inv, made)

        def scattered(act):
            @pl.loop(1, PIECES)
            def _(p):
                act(scatter_copy(0, p, made, land, scatter_send, scatter_recv, row, core))

            @pl.loop(0, PIECES)
            def _(p):
                act(scatter_copy(1, p, made, land, scatter_send, scatter_recv, row, core))

        scattered(lambda copy: copy.start())
        piece_out[...] = made[piece_rows(0, 0, 0, made.shape[0]), :]

        @pl.when(col == 0)
        def _():
            before_copy.wait_send()

        scattered(lambda copy: copy.wait_send())

    @pl.when(col >= 2)
    def _():
        load_others.start()
        load_value.wait()
        source_row = jnp.where(x_hi == 0, row, 1 - row)
        greet(source_row, core)
        pl.semaphore_wait(pltpu.get_barrier_semaphore(), 1)
        scatter_copy(0, piece, made, land, scatter_send, scatter_recv, row, core).wait_recv()
        piece_out[...] = land[...]

    load_others.wait()


def solve_pieces(rhs, inverse, own, got, after):
    half, block = rhs.shape[0], inverse.shape[1]
    length = half // (2 * PIECES)
    return pl.pallas_call(
        solve_kernel,
        out_shape=(
            pltpu.VMEM(rhs.shape, rhs.dtype),
            pltpu.VMEM((length, block), jnp.bfloat16),
        ),
        in_specs=[HBM] * 2 + [VMEM] * 2 + [ANY],
        out_specs=(VMEM, VMEM),
        scratch_shapes=[
            pltpu.VMEM((block, block), jnp.bfloat16),
            pltpu.VMEM((half, block), jnp.bfloat16),
            pltpu.VMEM((half, block), jnp.bfloat16),
            pltpu.VMEM((length, block), jnp.bfloat16),
            DMA((3,)), DMA((2, PIECES)), DMA, DMA, DMA,
        ],
        compiler_params=pltpu.CompilerParams(
            collective_id=0, has_side_effects=True, vmem_limit_bytes=20 << 20
        ),
        cost_estimate=BUSY,
        name="solve",
    )(rhs, inverse, own, got, after)


def gather_kernel(
    own_piece, taken, full, rest,
    mine, cross, x_send, x_recv, send_sem, recv_sem, core_send, core_recv,
):
    row, _, core, x_hi, z, y = place()
    half = cross.shape[0]
    has_cross = core == row
    steps = range(1, SIDE)

    for h, (kept, crossed) in enumerate(((own_piece, taken), (taken, own_piece))):
        @pl.when(x_hi == h)
        def _():
            here = piece_rows(h, z, y, half)
            mine[core, here, :] = kept[...]

            @pl.when(has_cross)
            def _():
                cross[here, :] = crossed[...]

    side = at(z, y, 1 - x_hi, core)
    greet(1 - row, side)
    greet(row, at(z, y, x_hi, 1 - core))
    for d in steps:
        greet(row, at(z, lax.rem(y + d, SIDE), x_hi, core))
        greet(row, at(lax.rem(z + d, SIDE), y, x_hi, core))
    pl.semaphore_wait(pltpu.get_barrier_semaphore(), 8)

    def x_copy(which, h, source):
        to = piece_rows(h, z, y, half)
        return remote(
            source, cross.at[to] if which else mine.at[core, to],
            x_send.at[which], x_recv.at[which], 1 - row, side,
        )

    for h, (kept, crossed) in enumerate(((own_piece, taken), (taken, own_piece))):
        @pl.when(x_hi == h)
        def _():
            x_copy(0, h, crossed).start()

            @pl.when(~has_cross)
            def _():
                x_copy(1, h, kept).start()

    for h in range(2):
        @pl.when(x_hi == 1 - h)
        def _():
            x_copy(0, h, taken).wait_recv()

            @pl.when(has_cross)
            def _():
                x_copy(1, h, taken).wait_recv()

    def copy(which, h, stage, d, back=False):
        buffer = cross if which else mine.at[core]
        along_y = (h == 0) == (stage == 0)
        turn = SIDE - d if back else d
        y_, z_ = (lax.rem(y + turn, SIDE), z) if along_y else (y, lax.rem(z + turn, SIDE))
        from_y, from_z = (y_, z_) if back else (y, z)
        if stage == 0:
            part = piece_rows(h, from_z, from_y, half)
        else:
            group = from_z if h == 0 else from_y
            part = pl.ds(
                pl.multiple_of(h * (half // 2) + group * (half // 8), half // 8), half // 8
            )
        y_to, z_to = (lax.rem(y + d, SIDE), z) if along_y else (y, lax.rem(z + d, SIDE))
        return remote(
            buffer.at[part], buffer.at[part],
            send_sem.at[which, h, stage, d - 1], recv_sem.at[which, h, stage, d - 1],
            row, at(z_to, y_to, x_hi, core),
        )

    def start(which, stage, h):
        for d in steps:
            copy(which, h, stage, d).start()

    def arrive(which, stage, h):
        for d in steps:
            copy(which, h, stage, d, True).wait_recv()

    for h in range(2):
        start(0, 0, h)

    @pl.when(has_cross)
    def _():
        for h in range(2):
            start(1, 0, h)

    for h in range(2):
        arrive(0, 0, h)
        start(0, 1, h)

    @pl.when(has_cross)
    def _():
        for h in range(2):
            arrive(1, 0, h)
            start(1, 1, h)

    buddy = at(z, y, x_hi, 1 - core)

    def share(which, h, take=False):
        part = pl.ds(h * (half // 2), half // 2)
        buffer = cross if which else mine.at[1 - core if take else core]
        return remote(
            buffer.at[part], buffer.at[part], core_send.at[which, h], core_recv.at[which, h],
            row, buddy,
        )

    for h in range(2):
        arrive(0, 1, h)
        share(0, h).start()

    @pl.when(has_cross)
    def _():
        for h in range(2):
            arrive(1, 1, h)
            share(1, h).start()

    for h in range(2):
        share(0, h, True).wait_recv()

    @pl.when(~has_cross)
    def _():
        for h in range(2):
            share(1, h, True).wait_recv()

    full[rows(row, half), :] = mine[row]
    full[rows(1 - row, half), :] = cross[...]
    rest[...] = mine[1 - row]

    def sent(which):
        for h in range(2):
            share(which, h).wait_send()
            for stage in range(2):
                for d in steps:
                    copy(which, h, stage, d).wait_send()

    sent(0)

    @pl.when(has_cross)
    def _():
        sent(1)

    x_copy(0, 0, taken).wait_send()

    @pl.when(~has_cross)
    def _():
        x_copy(1, 0, taken).wait_send()


def gather_pieces(piece, taken):
    length, block = piece.shape
    half = length * 2 * PIECES
    return pl.pallas_call(
        gather_kernel,
        out_shape=(
            pltpu.VMEM((2 * half, block), jnp.bfloat16),
            pltpu.VMEM((half, block), jnp.bfloat16),
        ),
        in_specs=[VMEM] * 2,
        out_specs=(VMEM, VMEM),
        scratch_shapes=[
            pltpu.VMEM((2, half, block), jnp.bfloat16),
            pltpu.VMEM((half, block), jnp.bfloat16),
            DMA((2,)), DMA((2,)), DMA((2, 2, 2, 3)), DMA((2, 2, 2, 3)), DMA((2, 2)), DMA((2, 2)),
        ],
        compiler_params=pltpu.CompilerParams(
            collective_id=2, has_side_effects=True, vmem_limit_bytes=12 << 20
        ),
        cost_estimate=BUSY,
        name="gather",
    )(piece, taken)


def chunk_of(length):
    return 256 if length % 256 == 0 else 128


def begin_kernel(held, full, rest, *refs, count, early):
    owns, parts, got = refs[:count], refs[count : count + early], refs[count + early]
    updated, solved, ahead, work, store_sem = refs[count + early + 1 :]
    row, col = lax.axis_index("row"), lax.axis_index("col")
    block = rest.shape[0]
    ready = work.shape[1]

    put_solved = pltpu.make_async_copy(full, solved, store_sem.at[0])
    put_solved.start()

    def store(index, start, length):
        part = pl.ds(start, length)
        return pltpu.make_async_copy(
            work.at[:, part], updated.at[:, part], store_sem.at[1 + index]
        )

    def step(i, start, mine, theirs):
        chunk = chunk_of(mine.shape[0])
        here = rows(i, chunk)
        column = pl.ds(pl.multiple_of(start + i * chunk, chunk), chunk)
        own = mine[here, :]
        if start == 0:
            own = jnp.where((col < 2) & (row >= col), jnp.zeros_like(own), own)
        total = lax.dot_general(
            full[rows(row, block), :], own, NT, preferred_element_type=jnp.float32
        )
        if theirs is None:
            ahead[:, pl.ds(pl.multiple_of(start + i * chunk - ready, chunk), chunk)] = (
                held[:, column] - total
            )
            return
        other = theirs[here, :]
        if start == 0:
            other = jnp.where(lax.rem(col, 2) == 1, got[here, :], other)
            other = jnp.where((col < 2) & (1 - row >= col), jnp.zeros_like(other), other)
        total += lax.dot_general(rest[...], other, NT, preferred_element_type=jnp.float32)
        work[:, column] = held[:, column] - total

    start = 0
    stores = []
    for index, mine in enumerate(owns):
        length = mine.shape[0]
        theirs = parts[index] if index < early else None
        pl.loop(0, length // chunk_of(length))(
            functools.partial(step, start=start, mine=mine, theirs=theirs)
        )
        if index < early:
            stores.append(store(index, start, length))
            stores[-1].start()
        start += length

    put_solved.wait()
    for copy in stores:
        copy.wait()


def begin(held, full, rest, owns, parts, got):
    half, rows_dev = held.shape
    ready = sum(part.shape[0] for part in parts)
    return pl.pallas_call(
        functools.partial(begin_kernel, count=len(owns), early=len(parts)),
        out_shape=(
            pltpu.HBM(held.shape, jnp.float32),
            pltpu.HBM(full.shape, full.dtype),
            pltpu.VMEM((half, rows_dev - ready), jnp.float32),
        ),
        in_specs=[VMEM] * (4 + len(owns) + len(parts)),
        out_specs=(HBM, HBM, VMEM),
        scratch_shapes=[
            pltpu.VMEM((half, ready), jnp.float32),
            DMA((1 + len(parts),)),
        ],
        compiler_params=pltpu.CompilerParams(vmem_limit_bytes=32 << 20),
        cost_estimate=BUSY,
        name="begin",
    )(held, full, rest, *owns, *parts, got)


def finish_kernel(start, offset, held, ahead, part, rest, updated, work, store_sem):
    length = part.shape[0]
    chunk = chunk_of(length)
    stores = []
    for j in range(length // chunk):
        here = pl.ds(j * chunk, chunk)
        total = lax.dot_general(
            rest[...], part[here, :], NT, preferred_element_type=jnp.float32
        )
        work[:, here] = ahead[:, pl.ds(offset + j * chunk, chunk)] - total
        stores.append(
            pltpu.make_async_copy(
                work.at[:, here], updated.at[:, pl.ds(start + j * chunk, chunk)], store_sem.at[j]
            )
        )
        stores[-1].start()
    for copy in stores:
        copy.wait()


def finish(updated, ahead, part, rest, start, offset):
    length = part.shape[0]
    return pl.pallas_call(
        functools.partial(finish_kernel, start, offset),
        out_shape=pltpu.HBM(updated.shape, updated.dtype),
        in_specs=[HBM, VMEM, VMEM, VMEM],
        out_specs=HBM,
        scratch_shapes=[
            pltpu.VMEM((ahead.shape[0], length), jnp.float32),
            DMA((length // chunk_of(length),)),
        ],
        input_output_aliases={0: 0},
        compiler_params=pltpu.CompilerParams(vmem_limit_bytes=12 << 20),
        cost_estimate=pl.CostEstimate(flops=10**9, bytes_accessed=10**6, transcendentals=0),
    )(updated, ahead, part, rest)


def swap(value, takes):
    col_count = lax.axis_size("col")
    pairs = [
        (row * col_count + col, (1 - row) * col_count + col)
        for row in range(2) for col in range(col_count) if takes(col)
    ]
    taken = lax.ppermute(value, ("row", "col"), pairs)
    return pltpu.with_memory_space_constraint(taken, pltpu.VMEM)


def shards(panel, rhs, inverse):
    panel, rhs, inverse = (
        pltpu.with_memory_space_constraint(value, pltpu.HBM) for value in (panel, rhs, inverse)
    )
    count = len(PARTS)
    starts = [sum(PARTS[:i]) for i in range(count)]
    sent, got = lead(panel, PARTS)
    arrived = [swap(sent[i], lambda col: i > 0 or (col % 2 == 0 and col > 0)) for i in range(count)]
    held, piece = solve_pieces(rhs, inverse, sent[0], got, sent[1])
    taken = swap(piece, lambda col: True)
    full, rest = gather_pieces(piece, taken)
    updated, solved, ahead = begin(held, full, rest, sent, arrived[:EARLY], got)
    for i in range(EARLY, count):
        updated = finish(updated, ahead, arrived[i], rest, starts[i], starts[i] - starts[EARLY])
    return solved, updated


def solution(mesh):
    return jax.shard_map(
        shards,
        mesh=mesh,
        in_specs=(P("col", "row"), P("row", "col"), P()),
        out_specs=(P(None, "row"), P("row", "col")),
        check_vma=False,
    )
```

```python
import functools

import jax
import jax.numpy as jnp
from jax import lax
from jax.experimental import pallas as pl
from jax.experimental.pallas import tpu as pltpu
from jax.sharding import PartitionSpec as P


MESH = pl.DeviceIdType.MESH
NT = (((1,), (1,)), ((), ()))
SIDE = 4
PIECES = SIDE * SIDE
PARTS = (512, 768, 1024, 512, 128, 128)
EARLY = 2
DMA = pltpu.SemaphoreType.DMA
HBM = pl.BlockSpec(memory_space=pltpu.HBM)
VMEM = pl.BlockSpec(memory_space=pltpu.VMEM)
ANY = pl.BlockSpec(memory_space=pl.ANY)
BUSY = pl.CostEstimate(flops=10**10, bytes_accessed=10**6, transcendentals=0)


def place():
    row = lax.axis_index("row")
    col = lax.axis_index("col")
    piece = col // 4
    return row, col, lax.rem(col, 2), lax.rem(col // 2, 2), piece // SIDE, lax.rem(piece, SIDE)


def at(z, y, x, core):
    return ((z * SIDE + y) * 2 + x) * 2 + core


def remote(src, dst, send, recv, row, col):
    return pltpu.make_async_remote_copy(
        src_ref=src, dst_ref=dst, send_sem=send, recv_sem=recv,
        device_id=(row, col), device_id_type=MESH,
    )


def greet(row, col):
    pl.semaphore_signal(
        pltpu.get_barrier_semaphore(), inc=1, device_id=(row, col), device_id_type=MESH
    )


def rows(i, length):
    return pl.ds(pl.multiple_of(i * length, length), length)


def lead_kernel(panel, *refs):
    *parts, got, load_sem, send_sem, recv_sem = refs
    row, col, core, _, _, _ = place()
    loads = []
    start = 0
    for i, part in enumerate(parts):
        loads.append(
            pltpu.make_async_copy(panel.at[pl.ds(start, part.shape[0])], part, load_sem.at[i])
        )
        start += part.shape[0]

    @pl.when(core == 1)
    def _():
        copy = remote(panel.at[pl.ds(0, got.shape[0])], got, send_sem, recv_sem, 1 - row, col)
        greet(1 - row, col)
        pl.semaphore_wait(pltpu.get_barrier_semaphore(), 1)
        copy.start()
        for load in loads:
            load.start()
        copy.wait()

    @pl.when(core == 0)
    def _():
        for load in loads:
            load.start()

    for load in loads:
        load.wait()


def lead(panel, lengths):
    parts = [pltpu.VMEM((length, panel.shape[1]), panel.dtype) for length in lengths]
    *parts, got = pl.pallas_call(
        lead_kernel,
        out_shape=(*parts, parts[0]),
        in_specs=[HBM],
        out_specs=(VMEM,) * (len(parts) + 1),
        scratch_shapes=[DMA((len(lengths),)), DMA, DMA],
        compiler_params=pltpu.CompilerParams(
            collective_id=1, has_side_effects=True, vmem_limit_bytes=8 << 20
        ),
        name="lead",
    )(panel)
    return parts, got


def solve(value, before, below, inv, made):
    rest = value[:, : made.shape[1]]
    if below is not None:
        rest = rest - lax.dot_general(
            before[...], below[...], NT, preferred_element_type=jnp.float32
        )
    high = rest.astype(jnp.bfloat16)
    rest = rest - high.astype(jnp.float32)
    middle = rest.astype(jnp.bfloat16)
    low = (rest - middle.astype(jnp.float32)).astype(jnp.bfloat16)
    total = lax.dot_general(low, inv[...], NT, preferred_element_type=jnp.float32)
    total += lax.dot_general(middle, inv[...], NT, preferred_element_type=jnp.float32)
    total += lax.dot_general(high, inv[...], NT, preferred_element_type=jnp.float32)
    made[...] = total.astype(jnp.bfloat16)


def piece_rows(h, z, y, half):
    length = half // (2 * PIECES)
    index = z * SIDE + y if h == 0 else y * SIDE + z
    return pl.ds(pl.multiple_of(h * (half // 2) + index * length, length), length)


def scatter_copy(h, p, made, land, send, recv, row, core):
    source = made.at[piece_rows(h, p // SIDE, lax.rem(p, SIDE), made.shape[0])]
    to_row = row if h == 0 else 1 - row
    return remote(source, land, send.at[h, p], recv, to_row, p * 4 + 2 * h + core)


def solve_kernel(
    rhs, inverse, own, got, after, held, piece_out,
    inv, made, before, land, load_sem, scatter_send, scatter_recv, before_send, before_recv,
):
    row, col, core, x_hi, _, _ = place()
    piece = col // 4
    block = inv.shape[0]
    load_value = pltpu.make_async_copy(
        rhs.at[:, pl.ds(0, block)], held.at[:, pl.ds(0, block)], load_sem.at[0]
    )
    others = pl.ds(block, rhs.shape[1] - block)
    load_others = pltpu.make_async_copy(rhs.at[:, others], held.at[:, others], load_sem.at[1])
    load_value.start()
    before_copy = remote(made, before, before_send, before_recv, row, 1)

    @pl.when(col < 2)
    def _():
        load_inv = pltpu.make_async_copy(inverse.at[core], inv, load_sem.at[2])
        load_inv.start()
        load_others.start()
        greet(row, 1 - core)

        @pl.loop(1, PIECES)
        def _(p):
            greet(row, p * 4 + core)

        @pl.loop(0, PIECES)
        def _(p):
            greet(1 - row, p * 4 + 2 + core)

        load_value.wait()
        load_inv.wait()

        @pl.when(col == 0)
        def _():
            solve(held, None, None, inv, made)

        pl.semaphore_wait(pltpu.get_barrier_semaphore(), 2 * PIECES)

        @pl.when(col == 0)
        def _():
            before_copy.start()

        @pl.when(col == 1)
        def _():
            before_copy.wait_recv()

            @pl.when(row == 0)
            def _():
                solve(held, before, own, inv, made)

            @pl.when(row == 1)
            def _():
                solve(held, before, got, inv, made)

        def scattered(act):
            @pl.loop(1, PIECES)
            def _(p):
                act(scatter_copy(0, p, made, land, scatter_send, scatter_recv, row, core))

            @pl.loop(0, PIECES)
            def _(p):
                act(scatter_copy(1, p, made, land, scatter_send, scatter_recv, row, core))

        scattered(lambda copy: copy.start())
        piece_out[...] = made[piece_rows(0, 0, 0, made.shape[0]), :]

        @pl.when(col == 0)
        def _():
            before_copy.wait_send()

        scattered(lambda copy: copy.wait_send())

    @pl.when(col >= 2)
    def _():
        load_others.start()
        load_value.wait()
        source_row = jnp.where(x_hi == 0, row, 1 - row)
        greet(source_row, core)
        pl.semaphore_wait(pltpu.get_barrier_semaphore(), 1)
        scatter_copy(0, piece, made, land, scatter_send, scatter_recv, row, core).wait_recv()
        piece_out[...] = land[...]

    load_others.wait()


def solve_pieces(rhs, inverse, own, got, after):
    half, block = rhs.shape[0], inverse.shape[1]
    length = half // (2 * PIECES)
    return pl.pallas_call(
        solve_kernel,
        out_shape=(
            pltpu.VMEM(rhs.shape, rhs.dtype),
            pltpu.VMEM((length, block), jnp.bfloat16),
        ),
        in_specs=[HBM] * 2 + [VMEM] * 2 + [ANY],
        out_specs=(VMEM, VMEM),
        scratch_shapes=[
            pltpu.VMEM((block, block), jnp.bfloat16),
            pltpu.VMEM((half, block), jnp.bfloat16),
            pltpu.VMEM((half, block), jnp.bfloat16),
            pltpu.VMEM((length, block), jnp.bfloat16),
            DMA((3,)), DMA((2, PIECES)), DMA, DMA, DMA,
        ],
        compiler_params=pltpu.CompilerParams(
            collective_id=0, has_side_effects=True, vmem_limit_bytes=20 << 20
        ),
        cost_estimate=BUSY,
        name="solve",
    )(rhs, inverse, own, got, after)


def gather_kernel(
    own_piece, taken, full, rest,
    mine, cross, x_send, x_recv, send_sem, recv_sem, core_send, core_recv,
):
    row, _, core, x_hi, z, y = place()
    half = cross.shape[0]
    has_cross = core == row
    steps = range(1, SIDE)

    for h, (kept, crossed) in enumerate(((own_piece, taken), (taken, own_piece))):
        @pl.when(x_hi == h)
        def _():
            here = piece_rows(h, z, y, half)
            mine[core, here, :] = kept[...]

            @pl.when(has_cross)
            def _():
                cross[here, :] = crossed[...]

    side = at(z, y, 1 - x_hi, core)
    greet(1 - row, side)
    greet(row, at(z, y, x_hi, 1 - core))
    for d in steps:
        greet(row, at(z, lax.rem(y + d, SIDE), x_hi, core))
        greet(row, at(lax.rem(z + d, SIDE), y, x_hi, core))
    pl.semaphore_wait(pltpu.get_barrier_semaphore(), 8)

    def x_copy(which, h, source):
        to = piece_rows(h, z, y, half)
        return remote(
            source, cross.at[to] if which else mine.at[core, to],
            x_send.at[which], x_recv.at[which], 1 - row, side,
        )

    for h, (kept, crossed) in enumerate(((own_piece, taken), (taken, own_piece))):
        @pl.when(x_hi == h)
        def _():
            x_copy(0, h, crossed).start()

            @pl.when(~has_cross)
            def _():
                x_copy(1, h, kept).start()

    for h in range(2):
        @pl.when(x_hi == 1 - h)
        def _():
            x_copy(0, h, taken).wait_recv()

            @pl.when(has_cross)
            def _():
                x_copy(1, h, taken).wait_recv()

    def copy(which, h, stage, d, back=False):
        buffer = cross if which else mine.at[core]
        along_y = (h == 0) == (stage == 0)
        turn = SIDE - d if back else d
        y_, z_ = (lax.rem(y + turn, SIDE), z) if along_y else (y, lax.rem(z + turn, SIDE))
        from_y, from_z = (y_, z_) if back else (y, z)
        if stage == 0:
            part = piece_rows(h, from_z, from_y, half)
        else:
            group = from_z if h == 0 else from_y
            part = pl.ds(
                pl.multiple_of(h * (half // 2) + group * (half // 8), half // 8), half // 8
            )
        y_to, z_to = (lax.rem(y + d, SIDE), z) if along_y else (y, lax.rem(z + d, SIDE))
        return remote(
            buffer.at[part], buffer.at[part],
            send_sem.at[which, h, stage, d - 1], recv_sem.at[which, h, stage, d - 1],
            row, at(z_to, y_to, x_hi, core),
        )

    def start(which, stage, h):
        for d in steps:
            copy(which, h, stage, d).start()

    def arrive(which, stage, h):
        for d in steps:
            copy(which, h, stage, d, True).wait_recv()

    for h in range(2):
        start(0, 0, h)

    @pl.when(has_cross)
    def _():
        for h in range(2):
            start(1, 0, h)

    for h in range(2):
        arrive(0, 0, h)
        start(0, 1, h)

    @pl.when(has_cross)
    def _():
        for h in range(2):
            arrive(1, 0, h)
            start(1, 1, h)

    buddy = at(z, y, x_hi, 1 - core)

    def share(which, h, take=False):
        part = pl.ds(h * (half // 2), half // 2)
        buffer = cross if which else mine.at[1 - core if take else core]
        return remote(
            buffer.at[part], buffer.at[part], core_send.at[which, h], core_recv.at[which, h],
            row, buddy,
        )

    for h in range(2):
        arrive(0, 1, h)
        share(0, h).start()

    @pl.when(has_cross)
    def _():
        for h in range(2):
            arrive(1, 1, h)
            share(1, h).start()

    for h in range(2):
        share(0, h, True).wait_recv()

    @pl.when(~has_cross)
    def _():
        for h in range(2):
            share(1, h, True).wait_recv()

    full[rows(row, half), :] = mine[row]
    full[rows(1 - row, half), :] = cross[...]
    rest[...] = mine[1 - row]

    def sent(which):
        for h in range(2):
            share(which, h).wait_send()
            for stage in range(2):
                for d in steps:
                    copy(which, h, stage, d).wait_send()

    sent(0)

    @pl.when(has_cross)
    def _():
        sent(1)

    x_copy(0, 0, taken).wait_send()

    @pl.when(~has_cross)
    def _():
        x_copy(1, 0, taken).wait_send()


def gather_pieces(piece, taken):
    length, block = piece.shape
    half = length * 2 * PIECES
    return pl.pallas_call(
        gather_kernel,
        out_shape=(
            pltpu.VMEM((2 * half, block), jnp.bfloat16),
            pltpu.VMEM((half, block), jnp.bfloat16),
        ),
        in_specs=[VMEM] * 2,
        out_specs=(VMEM, VMEM),
        scratch_shapes=[
            pltpu.VMEM((2, half, block), jnp.bfloat16),
            pltpu.VMEM((half, block), jnp.bfloat16),
            DMA((2,)), DMA((2,)), DMA((2, 2, 2, 3)), DMA((2, 2, 2, 3)), DMA((2, 2)), DMA((2, 2)),
        ],
        compiler_params=pltpu.CompilerParams(
            collective_id=2, has_side_effects=True, vmem_limit_bytes=12 << 20
        ),
        cost_estimate=BUSY,
        name="gather",
    )(piece, taken)


def chunk_of(length):
    return 256 if length % 256 == 0 else 128


def begin_kernel(held, full, rest, *refs, count, early):
    owns, parts, got = refs[:count], refs[count : count + early], refs[count + early]
    updated, solved, ahead, work, store_sem = refs[count + early + 1 :]
    row, col = lax.axis_index("row"), lax.axis_index("col")
    block = rest.shape[0]
    ready = work.shape[1]

    put_solved = pltpu.make_async_copy(full, solved, store_sem.at[0])
    put_solved.start()

    def store(index, start, length):
        part = pl.ds(start, length)
        return pltpu.make_async_copy(
            work.at[:, part], updated.at[:, part], store_sem.at[1 + index]
        )

    def step(i, start, mine, theirs):
        chunk = chunk_of(mine.shape[0])
        here = rows(i, chunk)
        column = pl.ds(pl.multiple_of(start + i * chunk, 128), chunk)
        own = mine[here, :]
        if start == 0:
            own = jnp.where((col < 2) & (row >= col), jnp.zeros_like(own), own)
        total = lax.dot_general(
            full[rows(row, block), :], own, NT, preferred_element_type=jnp.float32
        )
        if theirs is None:
            ahead[:, pl.ds(pl.multiple_of(start + i * chunk - ready, 128), chunk)] = (
                held[:, column] - total
            )
            return
        other = theirs[here, :]
        if start == 0:
            other = jnp.where(lax.rem(col, 2) == 1, got[here, :], other)
            other = jnp.where((col < 2) & (1 - row >= col), jnp.zeros_like(other), other)
        total += lax.dot_general(rest[...], other, NT, preferred_element_type=jnp.float32)
        work[:, column] = held[:, column] - total

    start = 0
    stores = []
    for index, mine in enumerate(owns):
        length = mine.shape[0]
        theirs = parts[index] if index < early else None
        pl.loop(0, length // chunk_of(length))(
            functools.partial(step, start=start, mine=mine, theirs=theirs)
        )
        if index < early:
            stores.append(store(index, start, length))
            stores[-1].start()
        start += length

    put_solved.wait()
    for copy in stores:
        copy.wait()


def begin(held, full, rest, owns, parts, got):
    half, rows_dev = held.shape
    ready = sum(part.shape[0] for part in parts)
    return pl.pallas_call(
        functools.partial(begin_kernel, count=len(owns), early=len(parts)),
        out_shape=(
            pltpu.HBM(held.shape, jnp.float32),
            pltpu.HBM(full.shape, full.dtype),
            pltpu.VMEM((half, rows_dev - ready), jnp.float32),
        ),
        in_specs=[VMEM] * (4 + len(owns) + len(parts)),
        out_specs=(HBM, HBM, VMEM),
        scratch_shapes=[
            pltpu.VMEM((half, ready), jnp.float32),
            DMA((1 + len(parts),)),
        ],
        compiler_params=pltpu.CompilerParams(vmem_limit_bytes=32 << 20),
        cost_estimate=BUSY,
        name="begin",
    )(held, full, rest, *owns, *parts, got)


def finish_kernel(start, offset, held, ahead, part, rest, updated, work, store_sem):
    length = part.shape[0]
    chunk = chunk_of(length)
    stores = []
    for j in range(length // chunk):
        here = pl.ds(j * chunk, chunk)
        total = lax.dot_general(
            rest[...], part[here, :], NT, preferred_element_type=jnp.float32
        )
        work[:, here] = ahead[:, pl.ds(offset + j * chunk, chunk)] - total
        stores.append(
            pltpu.make_async_copy(
                work.at[:, here], updated.at[:, pl.ds(start + j * chunk, chunk)], store_sem.at[j]
            )
        )
        stores[-1].start()
    for copy in stores:
        copy.wait()


def finish(updated, ahead, part, rest, start, offset):
    length = part.shape[0]
    return pl.pallas_call(
        functools.partial(finish_kernel, start, offset),
        out_shape=pltpu.HBM(updated.shape, updated.dtype),
        in_specs=[HBM, VMEM, VMEM, VMEM],
        out_specs=HBM,
        scratch_shapes=[
            pltpu.VMEM((ahead.shape[0], length), jnp.float32),
            DMA((length // chunk_of(length),)),
        ],
        input_output_aliases={0: 0},
        compiler_params=pltpu.CompilerParams(vmem_limit_bytes=12 << 20),
        cost_estimate=pl.CostEstimate(flops=10**9, bytes_accessed=10**6, transcendentals=0),
    )(updated, ahead, part, rest)


def swap(value, takes):
    col_count = lax.axis_size("col")
    pairs = [
        (row * col_count + col, (1 - row) * col_count + col)
        for row in range(2) for col in range(col_count) if takes(col)
    ]
    taken = lax.ppermute(value, ("row", "col"), pairs)
    return pltpu.with_memory_space_constraint(taken, pltpu.VMEM)


def shards(panel, rhs, inverse):
    panel, rhs, inverse = (
        pltpu.with_memory_space_constraint(value, pltpu.HBM) for value in (panel, rhs, inverse)
    )
    count = len(PARTS)
    starts = [sum(PARTS[:i]) for i in range(count)]
    sent, got = lead(panel, PARTS)
    arrived = [swap(sent[i], lambda col: i > 0 or (col % 2 == 0 and col > 0)) for i in range(count)]
    held, piece = solve_pieces(rhs, inverse, sent[0], got, sent[1])
    taken = swap(piece, lambda col: True)
    full, rest = gather_pieces(piece, taken)
    updated, solved, ahead = begin(held, full, rest, sent, arrived[:EARLY], got)
    for i in range(EARLY, count):
        updated = finish(updated, ahead, arrived[i], rest, starts[i], starts[i] - starts[EARLY])
    return solved, updated


def solution(mesh):
    return jax.shard_map(
        shards,
        mesh=mesh,
        in_specs=(P("col", "row"), P("row", "col"), P()),
        out_specs=(P(None, "row"), P("row", "col")),
        check_vma=False,
    )
```
